32 devices in a mesh: seq: 16 (over z, y, x), tp: 2 (over core).
Axes of the slice: x: 2, y: 2, z: 4, core: 2. Of those that a mesh axis runs over, the one named last changes fastest.
Arguments:
- query_rows: bfloat16 [2048, 2048], P('seq', 'tp'), may hold values from -350 to 350
- key_rows: bfloat16 [2048, 512], P('seq', 'tp'), may hold values from -6 to 6
- stored_value_rows: bfloat16 [2048, 512], P('seq', 'tp'), may hold values from -6 to 6
- output_grad: bfloat16 [2048, 2048], P('seq', 'tp'), may hold values from -96 to 96
- layer_input: bfloat16 [2048, 4096], P('seq', 'tp'), may hold values from -6 to 6
- key_matrix: bfloat16 [4096, 512], P(None, 'tp'), may hold values from -0.09375 to 0.09375
- value_matrix: bfloat16 [4096, 512], P(None, 'tp'), may hold values from -0.09375 to 0.09375
- run_placement: int32 [16, 16], replicated, may hold values from 0 to 15, as said below
Outputs:
- query_grad: bfloat16 [2048, 2048], P('seq', 'tp')
- input_grad: bfloat16 [2048, 4096], P('seq', 'tp')
- key_weight_grad: float32 [4096, 512], P('seq', 'tp')
- value_weight_grad: float32 [4096, 512], P('seq', 'tp')
The draws below stay inside these ranges and needn't reach their ends.
Inputs may be any that keep to these rules, and one draw needn't show every extreme that they name: `run_placement`: row j gives, for each storing index d of seq, the slot within sequence block j of the 8 consecutive positions that d holds; every row is a permutation of 0 to 15.
All inputs are finite; a program needn't handle non-finite values.
Results may differ from the reference program's by a relative error of at most 0.0081.
Values may be sent and summed in bfloat16 or wider, within the bound.
A program may use at most 128 MiB of HBM per device.

```python
import math
import jax
import jax.numpy as jnp
from jax import lax

MODEL_WIDTH = 4096
HEAD_SIZE = 128
WINDOW_LENGTH = 4096
QUERY_HEADS = 16
KEY_VALUE_HEADS = 4
TOK_DEV = 128
SEQUENCE_TOKENS = 2048
N_SEQ = 16


def slot_table(key):
    row_keys = jax.random.split(jax.random.fold_in(key, 101), N_SEQ)
    return jax.vmap(lambda row_key: jax.random.permutation(row_key, N_SEQ))(row_keys).astype(jnp.int32)


def key_sample(key):
    start_offset = jnp.clip(jax.random.normal(jax.random.fold_in(key, 202), (SEQUENCE_TOKENS, KEY_VALUE_HEADS, HEAD_SIZE), jnp.float32), -4.0, 4.0)
    return start_offset


def draw_run_placement(key, part):
    return slot_table(key)


def draw_key_rows(key, part):
    return key_sample(key).reshape(SEQUENCE_TOKENS, KEY_VALUE_HEADS * HEAD_SIZE).astype(jnp.bfloat16)


def draw_query_rows(key, part):
    start_offset = jnp.clip(jax.random.normal(jax.random.fold_in(key, 303), (SEQUENCE_TOKENS, QUERY_HEADS * HEAD_SIZE), jnp.float32), -4.0, 4.0)
    return start_offset.astype(jnp.bfloat16)


def spiked(drawn, key, source, target, parts, factor):
    owner, partner = [(jnp.arange(drawn.shape[dim]) // (drawn.shape[dim] // parts)).reshape([-1 if axis == dim else 1 for axis in range(drawn.ndim)]) for dim in (source, target)]
    chosen = jax.random.permutation(key, parts)[partner]
    strong = (owner == chosen) | (owner == (partner + parts // 2) % parts)
    return jnp.where(strong, factor * drawn, drawn)


def level_of(own_key, dims, shards, low, largest):
    def one(dim, blocks):
        steps = jax.random.uniform(jax.random.fold_in(jax.random.fold_in(own_key, 6), dim), (blocks,), jnp.float32, low / len(shards), largest / len(shards))
        return jnp.repeat(jnp.exp(steps), dims[dim] // blocks).reshape((-1,) + (1,) * (len(dims) - dim - 1))

    level = one(*shards[0])
    for cut in shards[1:]:
        level = level * one(*cut)
    return level


def normal_values(key, dims, width, reach, cuts=(), kind=jnp.bfloat16):
    drawn = width * jax.random.normal(key, dims, jnp.float32)
    if cuts:
        drawn = drawn * level_of(key, dims, cuts, -0.22, 0.18)
    return jnp.clip(drawn, -reach, reach).astype(kind)


def gaussian_with(rng, extent, scale, bound, cuts, heavy, held_as=jnp.bfloat16):
    array = scale * jax.random.normal(rng, extent, jnp.float32)
    if cuts:
        array = array * level_of(rng, extent, cuts, -0.22, 0.18)
    return jnp.clip(spiked(array, jax.random.fold_in(rng, 3), *heavy), -bound, bound).astype(held_as)


def setup_inputs(seed: int = 0) -> dict:
    key_list = jax.random.split(jax.random.key(seed), 9)
    return {
        "query_rows": draw_query_rows(jax.random.fold_in(key_list[8], 71), 0),
        "key_rows": draw_key_rows(jax.random.fold_in(key_list[8], 71), 0),
        "stored_value_rows": normal_values(key_list[2], (SEQUENCE_TOKENS, KEY_VALUE_HEADS * HEAD_SIZE), 1.0, 6.0, ((0, 16), (1, 2))),
        "output_grad": normal_values(key_list[3], (SEQUENCE_TOKENS, QUERY_HEADS * HEAD_SIZE), 16.0, 96.0, ((0, 16), (1, 2))),
        "layer_input": gaussian_with(key_list[4], (SEQUENCE_TOKENS, MODEL_WIDTH), 1.0, 6.0, ((0, 16), (1, 2)), (0, 1, 16, 2.0)),
        "key_matrix": normal_values(key_list[5], (MODEL_WIDTH, KEY_VALUE_HEADS * HEAD_SIZE), MODEL_WIDTH ** -0.5, 0.09375, ((1, 2),)),
        "value_matrix": normal_values(key_list[6], (MODEL_WIDTH, KEY_VALUE_HEADS * HEAD_SIZE), MODEL_WIDTH ** -0.5, 0.09375, ((1, 2),)),
        "run_placement": draw_run_placement(jax.random.fold_in(key_list[8], 71), 0),
    }


masked_value = -1e+30

def to_sequence(matrix, run_placement):
    run_rows = TOK_DEV // N_SEQ
    columns = matrix.shape[1]
    stored = matrix.reshape(N_SEQ, N_SEQ, run_rows, columns).transpose(1, 0, 2, 3)
    inverse = jnp.argsort(run_placement, axis=1).astype(jnp.int32)
    picked = jnp.take_along_axis(stored, inverse[:, :, None, None], axis=1)
    return picked.reshape(SEQUENCE_TOKENS, columns)

def into_stored_order(matrix, run_placement):
    run_rows = TOK_DEV // N_SEQ
    columns = matrix.shape[1]
    blocks = matrix.reshape(N_SEQ, N_SEQ, run_rows, columns)
    picked = jnp.take_along_axis(blocks, run_placement.astype(jnp.int32)[:, :, None, None], axis=1)
    return picked.transpose(1, 0, 2, 3).reshape(SEQUENCE_TOKENS, columns)

def rounded(values):
    return lax.optimization_barrier(values.astype(jnp.bfloat16)).astype(jnp.float32)

def reference(query_rows, key_rows, stored_value_rows, output_grad, layer_input, key_matrix, value_matrix, run_placement):
    score_scale = 1.0 / math.sqrt(HEAD_SIZE)
    query_group = QUERY_HEADS // KEY_VALUE_HEADS
    queries = to_sequence(query_rows, run_placement)
    grads = to_sequence(output_grad, run_placement)
    empty_rows = jnp.zeros((WINDOW_LENGTH, KEY_VALUE_HEADS * HEAD_SIZE), jnp.bfloat16)
    padded_keys = jnp.concatenate([empty_rows, to_sequence(key_rows, run_placement)], axis=0)
    padded_values = jnp.concatenate([empty_rows, to_sequence(stored_value_rows, run_placement)], axis=0)
    window_keys = WINDOW_LENGTH + TOK_DEV

    def one_block(carry, block_index):
        leading_row = block_index * TOK_DEV
        q_block = lax.dynamic_slice_in_dim(queries, leading_row, TOK_DEV, 0).astype(jnp.float32).reshape(TOK_DEV, QUERY_HEADS, HEAD_SIZE)
        g_block = lax.dynamic_slice_in_dim(grads, leading_row, TOK_DEV, 0).astype(jnp.float32).reshape(TOK_DEV, QUERY_HEADS, HEAD_SIZE)
        key_block = lax.dynamic_slice_in_dim(padded_keys, leading_row, window_keys, 0).astype(jnp.float32).reshape(window_keys, KEY_VALUE_HEADS, HEAD_SIZE)
        value_block = lax.dynamic_slice_in_dim(padded_values, leading_row, window_keys, 0).astype(jnp.float32).reshape(window_keys, KEY_VALUE_HEADS, HEAD_SIZE)
        k_heads = jnp.repeat(key_block, query_group, axis=1)
        v_heads = jnp.repeat(value_block, query_group, axis=1)
        query_pos = leading_row + jnp.arange(TOK_DEV, dtype=jnp.int32)
        key_pos = leading_row - WINDOW_LENGTH + jnp.arange(window_keys, dtype=jnp.int32)
        in_window = (key_pos[None, :] <= query_pos[:, None]) & (key_pos[None, :] > query_pos[:, None] - WINDOW_LENGTH) & (key_pos[None, :] >= 0)
        logits = jnp.einsum('qhd,khd->hqk', q_block, k_heads) * score_scale
        row_top = lax.optimization_barrier(jnp.max(jnp.where(in_window[None], logits, masked_value), axis=2))
        exponent = jnp.where(in_window[None], jnp.exp(logits - row_top[:, :, None]), 0.0)
        row_total = lax.optimization_barrier(jnp.sum(exponent, axis=2))
        log_total = row_top + jnp.log(row_total)
        prob_grad = jnp.einsum('qhd,khd->hqk', g_block, v_heads)
        row_delta = lax.optimization_barrier(jnp.sum(exponent * prob_grad, axis=2)) / row_total
        probs = jnp.where(in_window[None], jnp.exp(logits - log_total[:, :, None]), 0.0)
        score_grad = probs * (prob_grad - row_delta[:, :, None])
        probs_b = rounded(probs)
        score_b = rounded(score_grad)
        query_part = (jnp.einsum('hqk,khd->qhd', score_b, k_heads) * score_scale).astype(jnp.bfloat16)
        key_portion = jnp.einsum('hqk,qhd->khd', score_b, q_block) * score_scale
        key_portion = key_portion.reshape(window_keys, KEY_VALUE_HEADS, query_group, HEAD_SIZE).sum(axis=2).reshape(window_keys, KEY_VALUE_HEADS * HEAD_SIZE)
        value_portion = jnp.einsum('hqk,qhd->khd', probs_b, g_block)
        value_portion = value_portion.reshape(window_keys, KEY_VALUE_HEADS, query_group, HEAD_SIZE).sum(axis=2).reshape(window_keys, KEY_VALUE_HEADS * HEAD_SIZE)
        update = jnp.concatenate([key_portion, value_portion], axis=1)
        current = lax.dynamic_slice_in_dim(carry, leading_row, window_keys, 0)
        carry = lax.dynamic_update_slice_in_dim(carry, current + update, leading_row, 0)
        return (carry, query_part.reshape(TOK_DEV, QUERY_HEADS * HEAD_SIZE))
    gradient_start = jnp.zeros((WINDOW_LENGTH + SEQUENCE_TOKENS, 2 * KEY_VALUE_HEADS * HEAD_SIZE), jnp.float32)
    final, query_parts = lax.scan(one_block, gradient_start, jnp.arange(N_SEQ, dtype=jnp.int32))
    key_value_pair = final[WINDOW_LENGTH:]
    key_gradient = into_stored_order(key_value_pair[:, :KEY_VALUE_HEADS * HEAD_SIZE].astype(jnp.bfloat16), run_placement)
    value_gradient = into_stored_order(key_value_pair[:, KEY_VALUE_HEADS * HEAD_SIZE:].astype(jnp.bfloat16), run_placement)
    query_grad = into_stored_order(query_parts.reshape(SEQUENCE_TOKENS, QUERY_HEADS * HEAD_SIZE), run_placement)
    key_weight_grad = jnp.dot(layer_input.T, key_gradient, preferred_element_type=jnp.float32)
    value_weight_grad = jnp.dot(layer_input.T, value_gradient, preferred_element_type=jnp.float32)
    input_grad = jnp.dot(key_gradient, key_matrix.T, preferred_element_type=jnp.float32)
    input_grad = (input_grad + jnp.dot(value_gradient, value_matrix.T, preferred_element_type=jnp.float32)).astype(jnp.bfloat16)
    return (query_grad, input_grad, key_weight_grad, value_weight_grad)
```

```python
import math

import jax
import jax.numpy as jnp
from jax import lax
from jax.experimental import pallas as pl
from jax.experimental.pallas import tpu as pltpu
from jax.sharding import PartitionSpec as P

HEAD_SIZE = 128
WINDOW_LENGTH = 4096
GROUP = 4
CHUNK = 512
MASKED = -1e30
NT = (((1,), (1,)), ((), ()))
NN = (((1,), (0,)), ((), ()))
TN = (((0,), (0,)), ((), ()))
MESH = pl.DeviceIdType.MESH


def dot(a, b, dims):
    return lax.dot_general(a, b, dims, preferred_element_type=jnp.float32)


def flip(index, bit):
    return index + bit - 2 * bit * ((index // bit) % 2)


def step_kernel(
    q_ref, g_ref, k_ref, v_ref, pos_ref, x_ref, km_ref, vm_ref,
    dq_ref, own_ref, pair_ref, kw_ref, vw_ref, km_out, vm_out,
    kv_ref, qb_ref, gb_ref, kpos_ref, s_ref, dp_ref, p_ref, ds_ref, dqb_ref, dqa_ref,
    sum_ref, give_ref, take_ref, zs_ref, land_ref, fin_ref, all_ref, cols_ref, acc_ref,
    plane_send, kv_recv, kvz_send, kvp_send, kvp_recv, qg_send, qg_recv,
    x_send, x_recv, side_send, side_recv, local_sem,
    give_send, give_recv, z_send, z_recv, col_send, ag_send, ag_recv, dq_send, dq_recv,
):
    n = lax.axis_size("seq")
    cores = lax.axis_size("tp")
    me = lax.axis_index("seq")
    tp = lax.axis_index("tp")
    parts, run, _ = q_ref.shape
    kv_local = k_ref.shape[2] // HEAD_SIZE
    plane = cores * kv_local
    pair = GROUP // cores
    depth = n // plane
    z = me // plane
    p = me % plane
    home = p // kv_local
    lane = p % kv_local
    block = plane * run
    keys = n * run
    wide = pair * block
    sub = min(keys, CHUNK)
    roomy = dp_ref.shape[0] > 1
    windowed = parts * keys > WINDOW_LENGTH
    features = x_ref.shape[2]
    half = n // cores
    x_width = cols_ref.shape[2]
    block_width = features // half
    scale = 1.0 / math.sqrt(HEAD_SIZE)
    power = scale * math.log2(math.e)
    other = {"seq": me, "tp": 1 - tp}

    barrier = pltpu.get_barrier_semaphore()
    for step in range(n):
        for core in range(cores):
            if step or core:
                pl.semaphore_signal(
                    barrier,
                    inc=1,
                    device_id={"seq": (me + step) % n, "tp": (tp + core) % cores},
                    device_id_type=MESH,
                )
    pl.semaphore_wait(barrier, n * cores - 1)

    sent = []

    def when(cond, action):
        if cond is None:
            action()
        else:
            pl.when(cond)(action)

    def send(src, dst, send_sem, recv_sem, device, cond=None):
        def copy():
            return pltpu.make_async_remote_copy(
                src_ref=src, dst_ref=dst, send_sem=send_sem, recv_sem=recv_sem,
                device_id=device, device_id_type=MESH,
            )

        when(cond, lambda: copy().start())
        sent.append((cond, lambda: copy().wait_send()))

    def arrive(dst, recv_sem, cond=None):
        def wait():
            pltpu.make_async_remote_copy(
                src_ref=dst, dst_ref=dst, send_sem=recv_sem, recv_sem=recv_sem,
                device_id=other, device_id_type=MESH,
            ).wait_recv()

        when(cond, wait)

    def rows_of(index, count):
        return pl.ds(pl.multiple_of(index * count, count), count)

    def lanes_of(index):
        return pl.ds(pl.multiple_of(index * HEAD_SIZE, HEAD_SIZE), HEAD_SIZE)

    def piece(role, source):
        return kv_ref.at[role, :, rows_of(source, run), :]

    for i in range(kv_local):
        head = tp * kv_local + i
        target = z * plane + head
        for role, ref in enumerate((k_ref, v_ref)):
            mine = (head == p) & (tp == role)
            cols = slice(i * HEAD_SIZE, (i + 1) * HEAD_SIZE)
            send(
                ref.at[:, :, cols], piece(role, me), plane_send.at[i, role], kv_recv.at[me],
                {"seq": target, "tp": role}, jnp.logical_not(mine),
            )

            @pl.when(mine)
            def _():
                kv_ref[role, :, rows_of(me, run), :] = ref[:, :, cols]

    for i in range(kv_local):
        head = tp * kv_local + i
        target = z * plane + head
        for u in range(cores):
            mine = (head == p) & (tp == u)
            for h in range(pair):
                first = (i * GROUP + u * pair + h) * HEAD_SIZE
                cols = slice(first, first + HEAD_SIZE)
                for w, (ref, buf) in enumerate(((q_ref, qb_ref), (g_ref, gb_ref))):
                    send(
                        ref.at[:, :, cols], buf.at[:, h, rows_of(p, run), :],
                        qg_send.at[w, i, u, h], qg_recv.at[w, p, h],
                        {"seq": target, "tp": u}, jnp.logical_not(mine),
                    )

                    @pl.when(mine)
                    def _():
                        buf[:, h, rows_of(p, run), :] = ref[:, :, cols]

    pos_t = jnp.transpose(pos_ref[...])
    for b in range(parts):
        for s in range(depth):
            column = pos_t[:, s * parts + b : s * parts + b + 1]
            kpos_ref[b, s * block : (s + 1) * block, :] = jnp.broadcast_to(column, (block, block))

    def both(source):
        place = piece(tp, source)
        send(place, place, kvz_send.at[0, source], kv_recv.at[source],
             {"seq": jnp.minimum(me + plane, n - 1), "tp": tp}, z + 1 < depth)
        send(place, place, kvz_send.at[1, source], kv_recv.at[source],
             {"seq": jnp.maximum(me - plane, 0), "tp": tp}, z > 0)
        send(place, place, kvp_send.at[source], kvp_recv.at[source], other)

    for j in range(plane):
        index = (p + j) % plane
        source = z * plane + index
        if j == 0:
            arrive(piece(tp, source), kv_recv.at[source], home != tp)
        else:
            arrive(piece(tp, source), kv_recv.at[source])
        both(source)

    for k in range(1, depth):
        for j in range(plane):
            index = (p + j) % plane
            for way in range(2):
                at = z - k if way == 0 else z + k
                valid = at >= 0 if way == 0 else at < depth
                onward = valid & (z + 1 < depth) if way == 0 else valid & (z > 0)
                source = jnp.clip(at, 0, depth - 1) * plane + index
                place = piece(tp, source)
                arrive(place, kv_recv.at[source], valid)
                to = jnp.minimum(me + plane, n - 1) if way == 0 else jnp.maximum(me - plane, 0)
                send(place, place, kvz_send.at[way, source], kv_recv.at[source],
                     {"seq": to, "tp": tp}, onward)
                send(place, place, kvp_send.at[source], kvp_recv.at[source], other, valid)

    for w, buf in enumerate((qb_ref, gb_ref)):
        for j in range(plane):
            for h in range(pair):
                here = (p == j) & (home == tp)
                arrive(buf.at[:, h, j * run : (j + 1) * run, :], qg_recv.at[w, j, h],
                       jnp.logical_not(here))

    for i, (src, dst) in enumerate(((km_ref, km_out), (vm_ref, vm_out))):
        send(
            src.at[pl.ds(pl.multiple_of((1 - tp) * features, features), features), :], dst,
            side_send.at[i], side_recv.at[i], other,
        )

    def columns_of(target):
        start = ((target % half) * block_width) // x_width * x_width
        return x_ref.at[:, :, pl.ds(pl.multiple_of(start, x_width), x_width)]

    holder = tp == me // half
    own_columns = pltpu.make_async_copy(
        columns_of(me), cols_ref.at[:, rows_of(me, run), :], local_sem
    )

    @pl.when(holder)
    def _():
        own_columns.start()

    for slot in range(half):
        target = tp * half + (me + slot) % half
        send(
            columns_of(target), cols_ref.at[:, rows_of(me, run), :],
            x_send.at[slot], x_recv.at[me], {"seq": target, "tp": tp}, target != me,
        )

    for source in range(n):
        arrive(kv_ref.at[1 - tp, :, source * run : (source + 1) * run, :], kvp_recv.at[source])

    def lowest(a):
        low = 0
        while windowed and (a - low - 1) * keys + 1 >= WINDOW_LENGTH:
            low += 1
        return low

    tiles = [(a, b) for a in range(parts) for b in range(lowest(a), a + 1)]
    where = {tile: t for t, tile in enumerate(tiles)}

    def sweep(body, carry):
        if keys == sub:
            return body(slice(0, keys), carry)
        return lax.fori_loop(0, keys // sub, lambda i, c: body(rows_of(i, sub), c), carry)

    inverse, delta = [], []
    for a in range(parts):
        qa = qb_ref[a].reshape(wide, HEAD_SIZE)
        ga = gb_ref[a].reshape(wide, HEAD_SIZE)
        qpos = pos_ref[pl.ds(z * parts + a, 1), :]
        lows = range(lowest(a), a + 1)
        top = jnp.full((1, wide), MASKED, jnp.float32)
        for b in lows:

            def scores(at, top):
                s = dot(kv_ref[0, b, at, :], qa, NT)
                if a == b or windowed:
                    kpos = kpos_ref[b, at, :]
                    seen = kpos <= qpos
                    if windowed:
                        seen = seen & (kpos > qpos - WINDOW_LENGTH)
                    s = jnp.concatenate(
                        [
                            jnp.where(seen, s[:, h * block : (h + 1) * block], MASKED)
                            for h in range(pair)
                        ],
                        axis=1,
                    )
                s_ref[where[a, b], at, :] = s
                return jnp.maximum(top, jnp.max(s, axis=0, keepdims=True))

            top = sweep(scores, top)
        carry = (jnp.zeros((1, wide), jnp.float32), jnp.zeros((1, wide), jnp.float32))
        for b in lows:

            def sums(at, carry):
                total, weighted = carry
                e = jnp.exp2((s_ref[where[a, b], at, :] - top) * power)
                dp = dot(kv_ref[1, b, at, :], ga, NT)
                s_ref[where[a, b], at, :] = e
                if roomy:
                    dp_ref[where[a, b], at, :] = dp
                return (
                    total + jnp.sum(e, axis=0, keepdims=True),
                    weighted + jnp.sum(e * dp, axis=0, keepdims=True),
                )

            carry = sweep(sums, carry)
        total, weighted = carry
        inverse.append(1.0 / total)
        delta.append(weighted / total)

    def backward(b):
        uppers = [a for a in range(parts) if (a, b) in where]
        lo, hi = uppers[0], uppers[-1] + 1
        d = b if roomy else 0
        for a in uppers:
            lanes = slice(a * wide, (a + 1) * wide)

            def grads(at, carry):
                prob = s_ref[where[a, b], at, :] * inverse[a]
                if roomy:
                    dp = dp_ref[where[a, b], at, :]
                else:
                    dp = dot(kv_ref[1, b, at, :], gb_ref[a].reshape(wide, HEAD_SIZE), NT)
                p_ref[at, lanes] = prob.astype(jnp.bfloat16)
                ds_ref[d, at, lanes] = (prob * (dp - delta[a])).astype(jnp.bfloat16)
                return carry

            sweep(grads, 0)
        lanes = slice(lo * wide, hi * wide)
        q_all = qb_ref[lo:hi].reshape((hi - lo) * wide, HEAD_SIZE)
        g_all = gb_ref[lo:hi].reshape((hi - lo) * wide, HEAD_SIZE)

        def products(at, carry):
            dk = dot(ds_ref[d, at, lanes], q_all, NN) * scale
            dv = dot(p_ref[at, lanes], g_all, NN)
            first = tp == 0
            sum_ref[b, at, :] = jnp.where(first, dk, dv)
            give_ref[b, at, :] = jnp.where(first, dv, dk).astype(jnp.bfloat16)
            return carry

        sweep(products, 0)
        send(give_ref.at[b], take_ref.at[b], give_send.at[b], give_recv.at[b], other)
        if not roomy:
            for a in uppers:
                query_sum(a, b)

    def query_sum(a, b):
        d = b if roomy else 0
        lanes = slice(a * wide, (a + 1) * wide)

        def add(at, acc):
            return acc + dot(kv_ref[0, b, at, :], ds_ref[d, at, lanes], TN)

        acc = sweep(add, jnp.zeros((HEAD_SIZE, wide), jnp.float32))
        if b == a:
            dqa_ref[a] = acc
        else:
            dqa_ref[a] += acc

    def cross(b):
        arrive(take_ref.at[b], give_recv.at[b])
        total = sum_ref[b] + take_ref[b].astype(jnp.float32)
        sum_ref[b] = total
        zs_ref[b] = total.astype(jnp.bfloat16)
        for k in range(1, depth):
            to = (z + k) % depth
            send(
                zs_ref.at[b, rows_of(to, block), :], land_ref.at[b, k],
                z_send.at[b, k], z_recv.at[b, k], {"seq": to * plane + p, "tp": tp},
            )

    out_col = tp * kv_local + lane

    def finish(b):
        total = sum_ref[b, rows_of(z, block), :]
        for k in range(1, depth):
            arrive(land_ref.at[b, k], z_recv.at[b, k])
            total = total + land_ref[b, k].astype(jnp.float32)
        fin_ref[b] = total.astype(jnp.bfloat16)
        place = all_ref.at[b, out_col, rows_of(z, block), :]
        slot = ag_recv.at[b, z, out_col]
        send(fin_ref.at[b], place, col_send.at[b, 0], slot, other, home != tp)
        for k in range(1, depth):
            to = (z + k) % depth
            send(fin_ref.at[b], place, col_send.at[b, k], slot, {"seq": to * plane + p, "tp": home})

        @pl.when(home == tp)
        def _():
            all_ref[b, out_col, rows_of(z, block), :] = fin_ref[b]

    owner = home == tp
    mate_lane = kv_local - 1 - lane
    near = {"seq": z * plane + flip(p, 1), "tp": tp}
    across = {"seq": z * plane + flip(p, 2), "tp": tp}

    def gathered(b, at, c):
        return all_ref.at[b, c, rows_of(at, block), :], ag_recv.at[b, at, c]

    def push(b):
        for k in range(depth):
            at = (z + k) % depth
            for role in range(cores):
                c = role * kv_local + lane
                place, slot = gathered(b, at, c)
                arrive(place, slot, owner & (tp != role) if k == 0 else owner)
                send(place, place, ag_send.at[b, at, c, 0], slot, near, owner)
                send(place, place, ag_send.at[b, at, c, 1], slot, across, owner)

    def relay(b):
        for k in range(depth):
            at = (z + k) % depth
            c = mate_lane
            place, slot = gathered(b, at, c)
            arrive(place, slot, owner)
            send(place, place, ag_send.at[b, at, c, 1], slot, across, owner)
            c = kv_local + lane
            place, slot = gathered(b, at, c)
            arrive(place, slot, jnp.logical_not(owner))
            send(place, place, ag_send.at[b, at, c, 0], slot, near, jnp.logical_not(owner))

    def collect(b):
        for k in range(depth):
            at = (z + k) % depth
            place, slot = gathered(b, at, kv_local + mate_lane)
            arrive(place, slot)
            for c in (lane, mate_lane):
                place, slot = gathered(b, at, c)
                arrive(place, slot, jnp.logical_not(owner))

    def weigh(b, first):
        grads = [all_ref[b, c] for c in range(cores * kv_local)]
        part = dot(cols_ref[b], jnp.concatenate(grads, axis=1), TN)
        if first:
            acc_ref[...] = part
        else:
            acc_ref[...] += part

    def columns():
        @pl.when(holder)
        def _():
            own_columns.wait()

        for step in range(1, n):
            source = (me + step) % n
            arrive(cols_ref.at[:, rows_of(source, run), :], x_recv.at[source], holder)
        send(cols_ref, cols_ref, side_send.at[2], side_recv.at[2], other, holder)
        arrive(cols_ref, side_recv.at[2], jnp.logical_not(holder))

    def queries():
        for a in range(parts):
            if roomy:
                for b in reversed(range(lowest(a), a + 1)):
                    query_sum(a, b)
            out = (jnp.transpose(dqa_ref[a]) * scale).astype(jnp.bfloat16)
            dqb_ref[a] = out.reshape(pair, block, HEAD_SIZE)
        for j in range(plane):
            for h in range(pair):
                cols = lanes_of(lane * GROUP + tp * pair + h)
                mine = (p == j) & (home == tp)
                src = dqb_ref.at[:, h, j * run : (j + 1) * run, :]
                send(
                    src, dq_ref.at[:, :, cols], dq_send.at[h, j], dq_recv.at[lane, tp, h],
                    {"seq": z * plane + j, "tp": home}, jnp.logical_not(mine),
                )

                @pl.when(mine)
                def _():
                    dq_ref[:, :, cols] = dqb_ref[:, h, j * run : (j + 1) * run, :]

    last = parts - 1
    for tick in range(parts + 2):
        for level, stage in enumerate((backward, cross, finish)):
            b = last - (tick - level)
            if 0 <= b <= last:
                stage(b)
        if tick >= 2:
            push(last - (tick - 2))
        if tick == parts - 1:
            queries()
    for b in reversed(range(parts)):
        relay(b)
    columns()
    for b in reversed(range(parts)):
        collect(b)
        weigh(b, b == last)

    own_rows = rows_of(me, run)
    send(all_ref.at[:, :, own_rows, :], pair_ref, side_send.at[3], side_recv.at[3], other)
    own_ref[...] = all_ref[:, :, own_rows, :]
    middle = kv_local * HEAD_SIZE
    kw_ref[...] = acc_ref[:, :middle]
    vw_ref[...] = acc_ref[:, middle:]

    for i in range(kv_local):
        for u in range(cores):
            for h in range(pair):
                first = (i * GROUP + u * pair + h) * HEAD_SIZE
                here = (p == tp * kv_local + i) & (tp == u)
                arrive(dq_ref.at[:, :, first : first + HEAD_SIZE], dq_recv.at[i, u, h],
                       jnp.logical_not(here))
    for i, dst in enumerate((km_out, vm_out)):
        arrive(dst, side_recv.at[i])
    arrive(pair_ref, side_recv.at[3])
    for cond, wait in sent:
        when(cond, wait)


def step(n, q, g, k, v, pos, x, km, vm):
    parts, run, width = q.shape
    kv_width = k.shape[2]
    kv_local = kv_width // HEAD_SIZE
    features = x.shape[2]
    heads = width // HEAD_SIZE
    cores = km.shape[0] // features
    plane = cores * kv_local
    pair = GROUP // cores
    depth = n // plane
    block = plane * run
    keys = n * run
    wide = pair * block
    x_width = max(cores * features // n, 128)
    roomy = parts * keys <= 4096
    tiles = parts * (parts + 1) // 2
    vmem = pl.BlockSpec(memory_space=pltpu.VMEM)
    hbm = pl.BlockSpec(memory_space=pl.ANY)
    kind = jnp.bfloat16
    real = jnp.float32
    dma = pltpu.SemaphoreType.DMA
    return pl.pallas_call(
        step_kernel,
        out_shape=(
            jax.ShapeDtypeStruct((parts, run, width), kind),
            jax.ShapeDtypeStruct((parts, 2 * kv_local, run, HEAD_SIZE), kind),
            jax.ShapeDtypeStruct((parts, 2 * kv_local, run, HEAD_SIZE), kind),
            jax.ShapeDtypeStruct((x_width, kv_width), real),
            jax.ShapeDtypeStruct((x_width, kv_width), real),
            jax.ShapeDtypeStruct((features, kv_width), kind),
            jax.ShapeDtypeStruct((features, kv_width), kind),
        ),
        in_specs=[vmem] * 5 + [hbm] * 3,
        out_specs=(vmem, vmem, vmem, vmem, vmem, hbm, hbm),
        scratch_shapes=[
            pltpu.VMEM((2, parts, keys, HEAD_SIZE), kind),
            pltpu.VMEM((parts, pair, block, HEAD_SIZE), kind),
            pltpu.VMEM((parts, pair, block, HEAD_SIZE), kind),
            pltpu.VMEM((parts, keys, block), real),
            pltpu.VMEM((tiles, keys, wide), real),
            pltpu.VMEM((tiles, keys, wide) if roomy else (1, 8, 128), real),
            pltpu.VMEM((keys, parts * wide), kind),
            pltpu.VMEM((parts if roomy else 1, keys, parts * wide), kind),
            pltpu.VMEM((parts, pair, block, HEAD_SIZE), kind),
            pltpu.VMEM((parts, HEAD_SIZE, wide), real),
            pltpu.VMEM((parts, keys, HEAD_SIZE), real),
            pltpu.VMEM((parts, keys, HEAD_SIZE), kind),
            pltpu.VMEM((parts, keys, HEAD_SIZE), kind),
            pltpu.VMEM((parts, keys, HEAD_SIZE), kind),
            pltpu.VMEM((parts, depth, block, HEAD_SIZE), kind),
            pltpu.VMEM((parts, block, HEAD_SIZE), kind),
            pltpu.VMEM((parts, 2 * kv_local, keys, HEAD_SIZE), kind),
            pltpu.VMEM((parts, keys, x_width), kind),
            pltpu.VMEM((x_width, 2 * kv_width), real),
            dma((kv_local, cores)),
            dma((n,)),
            dma((2, n)),
            dma((n,)),
            dma((n,)),
            dma((2, kv_local, cores, pair)),
            dma((2, plane, pair)),
            dma((n // cores,)),
            dma((n,)),
            dma((4,)),
            dma((4,)),
            dma,
            dma((parts,)),
            dma((parts,)),
            dma((parts, depth)),
            dma((parts, depth)),
            dma((parts, depth)),
            dma((parts, depth, cores * kv_local, 2)),
            dma((parts, depth, cores * kv_local)),
            dma((pair, plane)),
            dma((kv_local, cores, pair)),
        ],
        compiler_params=pltpu.CompilerParams(
            vmem_limit_bytes=63 * 2**20, collective_id=0, has_side_effects=True
        ),
    )(q, g, k, v, pos, x, km, vm)


def positions(run_placement, rows_here, parts):
    seq_count = run_placement.shape[0]
    run_rows = rows_here // seq_count
    block = jnp.arange(seq_count, dtype=jnp.int32)[:, None] * rows_here
    start = jnp.transpose(block + run_placement * run_rows)
    pos = start[:, :, None] + jnp.arange(run_rows, dtype=jnp.int32)
    plane = parts
    pos = pos.reshape(seq_count // plane, plane, parts, rows_here // parts)
    pos = jnp.transpose(pos, (0, 2, 1, 3)).reshape(seq_count, rows_here)
    return pos.astype(jnp.float32)


def local(
    query_rows,
    key_rows,
    stored_value_rows,
    output_grad,
    layer_input,
    key_matrix,
    value_matrix,
    run_placement,
):
    seq_index = lax.axis_index("seq")
    tp_index = lax.axis_index("tp")
    seq_count = run_placement.shape[0]
    rows_here = query_rows.shape[0]
    kv_width = key_rows.shape[1]
    features = layer_input.shape[1]
    parts = (key_matrix.shape[0] // features) * (kv_width // HEAD_SIZE)

    def cut(array):
        return array.reshape(parts, rows_here // parts, array.shape[1])

    query_grad, kv_grad, kv_mate, key_weight, value_weight, key_far, value_far = step(
        seq_count,
        cut(query_rows),
        cut(output_grad),
        cut(key_rows),
        cut(stored_value_rows),
        positions(run_placement, rows_here, parts),
        cut(layer_input),
        key_matrix,
        value_matrix,
    )
    kv_grad = jnp.swapaxes(kv_grad, 1, 2).reshape(rows_here, 2 * kv_width)
    kv_mate = jnp.swapaxes(kv_mate, 1, 2).reshape(rows_here, 2 * kv_width)
    key_near = lax.dynamic_slice_in_dim(key_matrix, tp_index * features, features, 0)
    value_near = lax.dynamic_slice_in_dim(value_matrix, tp_index * features, features, 0)
    input_grad = (
        dot(kv_grad[:, :kv_width], key_near, NT)
        + dot(kv_grad[:, kv_width:], value_near, NT)
        + dot(kv_mate[:, :kv_width], key_far, NT)
        + dot(kv_mate[:, kv_width:], value_far, NT)
    ).astype(jnp.bfloat16)
    block_width = 2 * features // seq_count
    if key_weight.shape[0] != block_width:
        shift = (seq_index * block_width) % key_weight.shape[0]
        key_weight = lax.dynamic_slice_in_dim(key_weight, shift, block_width, 0)
        value_weight = lax.dynamic_slice_in_dim(value_weight, shift, block_width, 0)
    return (query_grad.reshape(query_rows.shape), input_grad, key_weight, value_weight)


def solution(mesh):
    placed = (P("seq", "tp"),) * 5 + (P(None, "tp"), P(None, "tp"), P())
    return jax.shard_map(
        local,
        mesh=mesh,
        in_specs=placed,
        out_specs=(P("seq", "tp"),) * 4,
        check_vma=False,
    )
```

```python
import math

import jax
import jax.numpy as jnp
from jax import lax
from jax.experimental import pallas as pl
from jax.experimental.pallas import tpu as pltpu
from jax.sharding import PartitionSpec as P

HEAD_SIZE = 128
WINDOW_LENGTH = 4096
GROUP = 4
CHUNK = 512
MASKED = -1e30
NT = (((1,), (1,)), ((), ()))
NN = (((1,), (0,)), ((), ()))
TN = (((0,), (0,)), ((), ()))
MESH = pl.DeviceIdType.MESH


def dot(a, b, dims):
    return lax.dot_general(a, b, dims, preferred_element_type=jnp.float32)


def flip(index, bit):
    return index + bit - 2 * bit * ((index // bit) % 2)


def visible(parts, keys):
    return [
        (a, b)
        for a in range(parts)
        for b in range(a + 1)
        if (a - b - 1) * keys + 1 < WINDOW_LENGTH
    ]


def step_kernel(
    q_ref, g_ref, k_ref, v_ref, pos_ref, x_ref, km_ref, vm_ref,
    dq_out, ig_out, kw_out, vw_out,
    kv_ref, qb_ref, gb_ref, kpos_ref, s_ref, dp_ref, p_ref, ds_ref, dqb_ref, dqa_ref,
    sum_ref, give_ref, take_ref, land_ref, fin_ref, all_ref, cols_ref, acc_ref,
    pair_ref, near_ref, far_ref, dq_ref, ig_ref,
    plane_send, kv_recv, kvz_send, kvp_send, kvp_recv, qg_send, qg_recv,
    x_send, x_recv, side_send, side_recv, local_sem,
    give_send, give_recv, z_send, z_recv, col_send,
    ag_send, push_recv, relay_recv, rest_recv, dq_send, dq_recv,
):
    n = lax.axis_size("seq")
    cores = lax.axis_size("tp")
    me = lax.axis_index("seq")
    tp = lax.axis_index("tp")
    parts, run, _ = q_ref.shape
    kv_local = k_ref.shape[2] // HEAD_SIZE
    plane = cores * kv_local
    pair = GROUP // cores
    depth = n // plane
    z = me // plane
    p = me % plane
    home = p // kv_local
    lane = p % kv_local
    block = plane * run
    keys = n * run
    wide = pair * block
    sub = min(keys, CHUNK)
    roomy = dp_ref.shape[0] > 1
    windowed = parts * keys > WINDOW_LENGTH
    features = x_ref.shape[2]
    half = n // cores
    x_width = cols_ref.shape[2]
    block_width = features // half
    scale = 1.0 / math.sqrt(HEAD_SIZE)
    power = scale * math.log2(math.e)
    other = {"seq": me, "tp": 1 - tp}

    owner = home == tp
    guest = jnp.logical_not(owner)

    def sum_all(count):
        each = count // parts
        high = next(c for c in range(1, each + 1) if each % c == 0 and each // c <= depth)
        return all_ref.at[:, :high, : each // high * block, :]

    barrier = pltpu.get_barrier_semaphore()
    for step in range(n):
        for core in range(cores):
            if step or core:
                pl.semaphore_signal(
                    barrier,
                    inc=1,
                    device_id={"seq": (me + step) % n, "tp": (tp + core) % cores},
                    device_id_type=MESH,
                )
    pl.semaphore_wait(barrier, n * cores - 1)

    def when(cond, action):
        if cond is None:
            action()
        else:
            pl.when(cond)(action)

    def send(src, dst, send_sem, recv_sem, device, cond=None):
        def copy():
            return pltpu.make_async_remote_copy(
                src_ref=src, dst_ref=dst, send_sem=send_sem, recv_sem=recv_sem,
                device_id=device, device_id_type=MESH,
            )

        when(cond, lambda: copy().start())

    def left(src, send_sem, cond=None):
        def wait():
            pltpu.make_async_remote_copy(
                src_ref=src, dst_ref=src, send_sem=send_sem, recv_sem=send_sem,
                device_id=other, device_id_type=MESH,
            ).wait_send()

        when(cond, wait)

    def arrive(dst, recv_sem, cond=None):
        def wait():
            pltpu.make_async_remote_copy(
                src_ref=dst, dst_ref=dst, send_sem=recv_sem, recv_sem=recv_sem,
                device_id=other, device_id_type=MESH,
            ).wait_recv()

        when(cond, wait)

    def rows_of(index, count):
        return pl.ds(pl.multiple_of(index * count, count), count)

    def lanes_of(index):
        return pl.ds(pl.multiple_of(index * HEAD_SIZE, HEAD_SIZE), HEAD_SIZE)

    def piece(role, source):
        return kv_ref.at[role, :, rows_of(source, run), :]

    for i in range(kv_local):
        head = tp * kv_local + i
        target = z * plane + head
        for role, ref in enumerate((k_ref, v_ref)):
            mine = (head == p) & (tp == role)
            cols = slice(i * HEAD_SIZE, (i + 1) * HEAD_SIZE)
            send(
                ref.at[:, :, cols], piece(role, me), plane_send.at[i, role], kv_recv.at[me],
                {"seq": target, "tp": role}, jnp.logical_not(mine),
            )

            @pl.when(mine)
            def _():
                kv_ref[role, :, rows_of(me, run), :] = ref[:, :, cols]

    for i in range(kv_local):
        head = tp * kv_local + i
        target = z * plane + head
        for u in range(cores):
            mine = (head == p) & (tp == u)
            for h in range(pair):
                first = (i * GROUP + u * pair + h) * HEAD_SIZE
                cols = slice(first, first + HEAD_SIZE)
                for w, (ref, buf) in enumerate(((q_ref, qb_ref), (g_ref, gb_ref))):
                    send(
                        ref.at[:, :, cols], buf.at[:, h, rows_of(p, run), :],
                        qg_send.at[w], qg_recv.at[w],
                        {"seq": target, "tp": u}, jnp.logical_not(mine),
                    )

                    @pl.when(mine)
                    def _():
                        buf[:, h, rows_of(p, run), :] = ref[:, :, cols]

    pos_t = jnp.transpose(pos_ref[...])
    for b in range(parts):
        for s in range(depth):
            column = pos_t[:, s * parts + b : s * parts + b + 1]
            kpos_ref[b, s * block : (s + 1) * block, :] = jnp.broadcast_to(column, (block, block))

    bits = [1 << e for e in range(depth.bit_length() - 1)]
    order = sorted(range(depth), key=lambda k: (bin(k).count("1"), -k))

    def layer(k):
        index = z
        for bit in bits:
            if k & bit:
                index = flip(index, bit)
        return index

    def lower(k):
        return [bit for bit in reversed(bits) if k == 0 or bit < (k & -k)]

    def pass_on(k):
        for j in range(plane):
            source = layer(k) * plane + (p + j) % plane
            place = piece(tp, source)
            arrive(place, kv_recv.at[source], home != tp if k + j == 0 else None)
            for bit in lower(k):
                send(place, place, kvz_send, kv_recv.at[source],
                     {"seq": flip(z, bit) * plane + p, "tp": tp})
            send(place, place, kvp_send, kvp_recv, other)

    relayed = [k for k in order if lower(k)]
    for k in relayed:
        pass_on(k)

    def half_of(src, core):
        return src.at[pl.ds(pl.multiple_of(core * features, features), features), :]

    nearby = []
    for i, src in enumerate((km_ref, vm_ref)):
        send(half_of(src, 1 - tp), far_ref.at[i], side_send.at[i], side_recv.at[i], other)
        nearby.append(pltpu.make_async_copy(half_of(src, tp), near_ref.at[i], local_sem.at[i]))
        nearby[-1].start()

    def columns_of(target):
        start = ((target % half) * block_width) // x_width * x_width
        return x_ref.at[:, :, pl.ds(pl.multiple_of(start, x_width), x_width)]

    holder = tp == me // half
    own_columns = pltpu.make_async_copy(
        columns_of(me), cols_ref.at[:, rows_of(me, run), :], local_sem.at[2]
    )

    @pl.when(holder)
    def _():
        own_columns.start()

    for slot in range(half):
        target = tp * half + (me + half // 2 + slot) % half
        send(
            columns_of(target), cols_ref.at[:, rows_of(me, run), :],
            x_send, x_recv, {"seq": target, "tp": tp}, target != me,
        )

    for k in order:
        if k not in relayed:
            pass_on(k)

    fewer = (plane - 1) * run
    for w, buf in enumerate((qb_ref, gb_ref)):
        arrive(buf, qg_recv.at[w], guest)
        arrive(buf.at[:, :, :fewer, :], qg_recv.at[w], owner)
    arrive(kv_ref.at[1 - tp], kvp_recv)

    tiles = visible(parts, keys)

    def lowest(a):
        return min(b for c, b in tiles if c == a)

    where = {tile: t for t, tile in enumerate(tiles)}

    def sweep(body, carry):
        if keys == sub:
            return body(slice(0, keys), carry)
        return lax.fori_loop(0, keys // sub, lambda i, c: body(rows_of(i, sub), c), carry)

    inverse, delta = [], []
    for a in range(parts):
        qa = qb_ref[a].reshape(wide, HEAD_SIZE)
        ga = gb_ref[a].reshape(wide, HEAD_SIZE)
        qpos = pos_ref[pl.ds(z * parts + a, 1), :]
        lows = range(lowest(a), a + 1)
        top = jnp.full((1, wide), MASKED, jnp.float32)
        for b in lows:

            def scores(at, top):
                s = dot(kv_ref[0, b, at, :], qa, NT)
                if a == b or windowed:
                    kpos = kpos_ref[b, at, :]
                    seen = kpos <= qpos
                    if windowed:
                        seen = seen & (kpos > qpos - WINDOW_LENGTH)
                    s = jnp.concatenate(
                        [
                            jnp.where(seen, s[:, h * block : (h + 1) * block], MASKED)
                            for h in range(pair)
                        ],
                        axis=1,
                    )
                s_ref[where[a, b], at, :] = s
                return jnp.maximum(top, jnp.max(s, axis=0, keepdims=True))

            top = sweep(scores, top)
        carry = (jnp.zeros((1, wide), jnp.float32), jnp.zeros((1, wide), jnp.float32))
        for b in lows:

            def sums(at, carry):
                total, weighted = carry
                e = jnp.exp2((s_ref[where[a, b], at, :] - top) * power)
                dp = dot(kv_ref[1, b, at, :], ga, NT)
                s_ref[where[a, b], at, :] = e
                if roomy:
                    dp_ref[where[a, b], at, :] = dp
                return (
                    total + jnp.sum(e, axis=0, keepdims=True),
                    weighted + jnp.sum(e * dp, axis=0, keepdims=True),
                )

            carry = sweep(sums, carry)
        total, weighted = carry
        inverse.append(1.0 / total)
        delta.append(weighted / total)

    def backward(b):
        uppers = [a for a in range(parts) if (a, b) in where]
        lo, hi = uppers[0], uppers[-1] + 1
        d = b if roomy else 0
        for a in uppers:
            lanes = slice(a * wide, (a + 1) * wide)

            def grads(at, carry):
                prob = s_ref[where[a, b], at, :] * inverse[a]
                if roomy:
                    dp = dp_ref[where[a, b], at, :]
                else:
                    dp = dot(kv_ref[1, b, at, :], gb_ref[a].reshape(wide, HEAD_SIZE), NT)
                p_ref[at, lanes] = prob.astype(jnp.bfloat16)
                ds_ref[d, at, lanes] = (prob * (dp - delta[a])).astype(jnp.bfloat16)
                return carry

            sweep(grads, 0)
        lanes = slice(lo * wide, hi * wide)
        q_all = qb_ref[lo:hi].reshape((hi - lo) * wide, HEAD_SIZE)
        g_all = gb_ref[lo:hi].reshape((hi - lo) * wide, HEAD_SIZE)

        def products(at, carry):
            dk = dot(ds_ref[d, at, lanes], q_all, NN) * scale
            dv = dot(p_ref[at, lanes], g_all, NN)
            first = tp == 0
            sum_ref[b, at, :] = jnp.where(first, dk, dv)
            give_ref[b, at, :] = jnp.where(first, dv, dk).astype(jnp.bfloat16)
            return carry

        sweep(products, 0)
        send(give_ref.at[b], take_ref.at[b], give_send, give_recv.at[b], other)
        if not roomy:
            for a in uppers:
                query_sum(a, b)

    def query_sum(a, b):
        d = b if roomy else 0
        lanes = slice(a * wide, (a + 1) * wide)

        def add(at, acc):
            return acc + dot(kv_ref[0, b, at, :], ds_ref[d, at, lanes], TN)

        acc = sweep(add, jnp.zeros((HEAD_SIZE, wide), jnp.float32))
        if b == a:
            dqa_ref[a] = acc
        else:
            dqa_ref[a] += acc

    def exchange(b, e):
        bit = bits[e]
        first = depth - depth // bit
        for t in range(depth // (2 * bit)):
            to = flip(z, bit) % (2 * bit) + t * 2 * bit
            rows = rows_of(to, block)
            take_ref[b, rows, :] = sum_ref[b, rows, :].astype(jnp.bfloat16)
            send(
                take_ref.at[b, rows, :], land_ref.at[b, first + t], z_send,
                z_recv.at[b, e], {"seq": flip(z, bit) * plane + p, "tp": tp},
            )

    def cross(b):
        arrive(take_ref.at[b], give_recv.at[b])
        sum_ref[b] += take_ref[b].astype(jnp.float32)
        exchange(b, 0)

    def add_landed(b, e):
        bit = bits[e]
        count = depth // (2 * bit)
        first = depth - depth // bit
        arrive(land_ref.at[b, first : first + count], z_recv.at[b, e])
        for t in range(count):
            rows = rows_of(z % (2 * bit) + t * 2 * bit, block)
            sum_ref[b, rows, :] += land_ref[b, first + t].astype(jnp.float32)

    def fold(e):
        def go(b):
            add_landed(b, e - 1)
            exchange(b, e)

        return go

    out_col = tp * kv_local + lane

    def finish(b):
        add_landed(b, len(bits) - 1)
        fin_ref[b] = sum_ref[b, rows_of(z, block), :].astype(jnp.bfloat16)
        place = all_ref.at[b, out_col, rows_of(z, block), :]
        slot = push_recv.at[b, z]
        for bit in reversed(bits):
            send(fin_ref.at[b], place, col_send, slot,
                 {"seq": flip(z, bit) * plane + p, "tp": home})
        send(fin_ref.at[b], place, col_send, slot, other, guest)

        @pl.when(owner)
        def _():
            all_ref[b, out_col, rows_of(z, block), :] = fin_ref[b]

    mate_lane = kv_local - 1 - lane
    near = {"seq": z * plane + flip(p, 1), "tp": tp}
    across = {"seq": z * plane + flip(p, 2), "tp": tp}

    def gathered(b, at, c):
        return all_ref.at[b, c, rows_of(at, block), :]

    def later(b, k):
        return rest_recv.at[b if k else parts]

    def push(b):
        for k in order:
            at = layer(k)
            slot = push_recv.at[b, at]
            arrive(all_ref.at[b, 0, : (1 if k == 0 else cores) * block, :], slot, owner)
            for role in range(cores):
                place = gathered(b, at, role * kv_local + lane)
                if k:
                    for bit in lower(k):
                        send(place, place, ag_send.at[0], slot,
                             {"seq": flip(z, bit) * plane + p, "tp": tp}, owner)
                turn, rest = relay_recv.at[b, k], later(b, k)
                send(place, place, ag_send.at[1], rest if role else turn, near, owner)
                send(place, place, ag_send.at[2], turn if role else rest, across, owner)

    def relay(b):
        for k in order:
            at = layer(k)
            turn, rest = relay_recv.at[b, k], later(b, k)
            arrive(all_ref.at[b, 0, :block, :], turn)
            place = gathered(b, at, mate_lane)
            send(place, place, ag_send.at[3], rest, across, owner)
            place = gathered(b, at, kv_local + lane)
            send(place, place, ag_send.at[3], rest, near, guest)

    def collect(b):
        count = (depth - 1) * block
        arrive(all_ref.at[b, 0, :count, :], rest_recv.at[b], owner)
        arrive(all_ref.at[b, :3, :count, :], rest_recv.at[b], guest)

    def weigh(b, first):
        grads = [all_ref[b, c] for c in range(cores * kv_local)]
        part = dot(cols_ref[b], jnp.concatenate(grads, axis=1), TN)
        if first:
            acc_ref[...] = part
        else:
            acc_ref[...] += part

    def columns():
        @pl.when(holder)
        def _():
            own_columns.wait()

        arrive(cols_ref.at[:, : (n - 1) * run, :], x_recv, holder)
        send(cols_ref, cols_ref, side_send.at[2], side_recv.at[2], other, holder)
        arrive(cols_ref, side_recv.at[2], jnp.logical_not(holder))

    def queries():
        for a in range(parts):
            if roomy:
                for b in reversed(range(lowest(a), a + 1)):
                    query_sum(a, b)
            out = (jnp.transpose(dqa_ref[a]) * scale).astype(jnp.bfloat16)
            dqb_ref[a] = out.reshape(pair, block, HEAD_SIZE)
        for j in range(plane):
            for h in range(pair):
                cols = lanes_of(lane * GROUP + tp * pair + h)
                mine = (p == j) & (home == tp)
                src = dqb_ref.at[:, h, j * run : (j + 1) * run, :]
                send(
                    src, dq_ref.at[:, :, cols], dq_send, dq_recv,
                    {"seq": z * plane + j, "tp": home}, jnp.logical_not(mine),
                )

                @pl.when(mine)
                def _():
                    dq_ref[:, :, cols] = dqb_ref[:, h, j * run : (j + 1) * run, :]

    own_rows = rows_of(me, run)
    leaving = []

    def put(src, dst):
        leaving.append(pltpu.make_async_copy(src, dst, local_sem.at[3 + len(leaving)]))
        leaving[-1].start()

    def answers():
        arrive(dqb_ref, dq_recv, guest)
        arrive(dqb_ref.at[:, :, :fewer, :], dq_recv, owner)
        put(dq_ref, dq_out)

    def swap():
        arrive(all_ref.at[:, 0, :block, :], rest_recv.at[parts], owner)
        arrive(all_ref.at[:, :3, :block, :], rest_recv.at[parts], guest)
        send(all_ref.at[:, :, own_rows, :], pair_ref, side_send.at[3], side_recv.at[3], other)

    def inputs():
        for copy in nearby:
            copy.wait()
        for i in range(2):
            arrive(far_ref.at[i], side_recv.at[i])
        arrive(pair_ref, side_recv.at[3])
        rows = parts * run
        grads = [all_ref[:, c, own_rows, :].reshape(rows, HEAD_SIZE) for c in range(2 * kv_local)]
        grads += [pair_ref[:, c].reshape(rows, HEAD_SIZE) for c in range(2 * kv_local)]
        grads = jnp.concatenate(grads, axis=1)
        for f in range(0, features, CHUNK):
            tile = slice(f, min(f + CHUNK, features))
            weights = [ref[i, tile, :] for ref in (near_ref, far_ref) for i in range(2)]
            out = dot(grads, jnp.concatenate(weights, axis=1), NT)
            ig_ref[:, tile] = out.astype(jnp.bfloat16)
        put(ig_ref, ig_out)

    stages = [backward, cross] + [fold(e) for e in range(1, len(bits))] + [finish, push]
    last = parts - 1
    for tick in range(last + len(stages)):
        for level, stage in enumerate(stages):
            b = last - (tick - level)
            if 0 <= b <= last:
                stage(b)
        if tick == last:
            queries()
    for b in reversed(range(parts)):
        relay(b)
    swap()
    columns()
    answers()
    for b in reversed(range(parts)):
        if b == 0:
            inputs()
        collect(b)
        weigh(b, b == last)

    middle = kv_local * HEAD_SIZE
    put(acc_ref.at[:, :middle], kw_out)
    put(acc_ref.at[:, middle:], vw_out)
    for copy in leaving:
        copy.wait()

    for i in range(kv_local):
        for role in range(cores):
            mine = (tp * kv_local + i == p) & (tp == role)
            left(piece(role, me), plane_send.at[i, role], jnp.logical_not(mine))
    for w, buf in ((0, qb_ref), (1, gb_ref)):
        left(buf, qg_send.at[w], guest)
        left(buf.at[:, :, :fewer, :], qg_send.at[w], owner)
    moves = sum(len(lower(k)) for k in order)
    left(kv_ref.at[0, :, : moves * block, :], kvz_send)
    left(kv_ref.at[0], kvp_send)
    left(cols_ref.at[:, : half * run, :], x_send, jnp.logical_not(holder))
    left(cols_ref.at[:, : (half - 1) * run, :], x_send, holder)
    left(cols_ref, side_send.at[2], holder)
    for i in range(2):
        left(far_ref.at[i], side_send.at[i])
    left(pair_ref, side_send.at[3])
    left(give_ref, give_send)
    left(take_ref.at[:, : (depth - 1) * block, :], z_send)
    left(dqb_ref, dq_send, guest)
    left(dqb_ref.at[:, :, :fewer, :], dq_send, owner)
    ways = len(bits)
    left(sum_all(ways * parts), col_send, owner)
    left(sum_all((ways + 1) * parts), col_send, guest)
    left(sum_all((moves - ways) * cores * parts), ag_send.at[0], owner)
    left(sum_all(depth * cores * parts), ag_send.at[1], owner)
    left(sum_all(depth * cores * parts), ag_send.at[2], owner)
    left(sum_all(depth * parts), ag_send.at[3])


def deliver_kernel(*refs):
    count = (len(refs) - 1) // 3
    ins, outs, held = refs[:count], refs[count : 2 * count], refs[2 * count : 3 * count]
    sems = refs[3 * count]
    moves = []
    for i in range(count):
        moves.append(pltpu.make_async_copy(ins[i], held[i], sems.at[0, i]))
        moves[-1].start()
    for i in range(count):
        moves[i].wait()
        moves.append(pltpu.make_async_copy(held[i], outs[i], sems.at[1, i]))
        moves[-1].start()
    for move in moves[count:]:
        move.wait()


def deliver(*arrays):
    hbm = pl.BlockSpec(memory_space=pl.ANY)
    count = len(arrays)
    return pl.pallas_call(
        deliver_kernel,
        out_shape=tuple(jax.ShapeDtypeStruct(a.shape, a.dtype) for a in arrays),
        in_specs=[hbm] * count,
        out_specs=(hbm,) * count,
        scratch_shapes=[pltpu.VMEM(a.shape, a.dtype) for a in arrays]
        + [pltpu.SemaphoreType.DMA((2, count))],
    )(*arrays)


def step(n, q, g, k, v, pos, x, km, vm):
    parts, run, width = q.shape
    kv_width = k.shape[2]
    kv_local = kv_width // HEAD_SIZE
    features = x.shape[2]
    heads = width // HEAD_SIZE
    cores = km.shape[0] // features
    plane = cores * kv_local
    pair = GROUP // cores
    depth = n // plane
    levels = depth.bit_length() - 1
    block = plane * run
    keys = n * run
    wide = pair * block
    x_width = max(cores * features // n, 128)
    roomy = parts * keys <= 4096
    tiles = len(visible(parts, keys))
    vmem = pl.BlockSpec(memory_space=pltpu.VMEM)
    hbm = pl.BlockSpec(memory_space=pl.ANY)
    kind = jnp.bfloat16
    real = jnp.float32
    dma = pltpu.SemaphoreType.DMA
    return pl.pallas_call(
        step_kernel,
        out_shape=(
            jax.ShapeDtypeStruct((parts, run, width), kind),
            jax.ShapeDtypeStruct((parts * run, features), kind),
            jax.ShapeDtypeStruct((x_width, kv_width), real),
            jax.ShapeDtypeStruct((x_width, kv_width), real),
        ),
        in_specs=[vmem] * 5 + [hbm] * 3,
        out_specs=(hbm,) * 4,
        scratch_shapes=[
            pltpu.VMEM((2, parts, keys, HEAD_SIZE), kind),
            pltpu.VMEM((parts, pair, block, HEAD_SIZE), kind),
            pltpu.VMEM((parts, pair, block, HEAD_SIZE), kind),
            pltpu.VMEM((parts, keys, block), real),
            pltpu.VMEM((tiles, keys, wide), real),
            pltpu.VMEM((tiles, keys, wide) if roomy else (1, 8, 128), real),
            pltpu.VMEM((keys, parts * wide), kind),
            pltpu.VMEM((parts if roomy else 1, keys, parts * wide), kind),
            pltpu.VMEM((parts, pair, block, HEAD_SIZE), kind),
            pltpu.VMEM((parts, HEAD_SIZE, wide), real),
            pltpu.VMEM((parts, keys, HEAD_SIZE), real),
            pltpu.VMEM((parts, keys, HEAD_SIZE), kind),
            pltpu.VMEM((parts, keys, HEAD_SIZE), kind),
            pltpu.VMEM((parts, depth - 1, block, HEAD_SIZE), kind),
            pltpu.VMEM((parts, block, HEAD_SIZE), kind),
            pltpu.VMEM((parts, 2 * kv_local, keys, HEAD_SIZE), kind),
            pltpu.VMEM((parts, keys, x_width), kind),
            pltpu.VMEM((x_width, 2 * kv_width), real),
            pltpu.VMEM((parts, 2 * kv_local, run, HEAD_SIZE), kind),
            pltpu.VMEM((2, features, kv_width), kind),
            pltpu.VMEM((2, features, kv_width), kind),
            pltpu.VMEM((parts, run, width), kind),
            pltpu.VMEM((parts * run, features), kind),
            dma((kv_local, cores)),
            dma((n,)),
            dma,
            dma,
            dma,
            dma((2,)),
            dma((2,)),
            dma,
            dma,
            dma((4,)),
            dma((4,)),
            dma((7,)),
            dma,
            dma((parts,)),
            dma,
            dma((parts, levels)),
            dma,
            dma((4,)),
            dma((parts, depth)),
            dma((parts, depth)),
            dma((parts + 1,)),
            dma,
            dma,
        ],
        compiler_params=pltpu.CompilerParams(
            vmem_limit_bytes=63 * 2**20, collective_id=0, has_side_effects=True
        ),
    )(q, g, k, v, pos, x, km, vm)


def positions(run_placement, rows_here, parts):
    seq_count = run_placement.shape[0]
    run_rows = rows_here // seq_count
    block = jnp.arange(seq_count, dtype=jnp.int32)[:, None] * rows_here
    start = jnp.transpose(block + run_placement * run_rows)
    pos = start[:, :, None] + jnp.arange(run_rows, dtype=jnp.int32)
    plane = parts
    pos = pos.reshape(seq_count // plane, plane, parts, rows_here // parts)
    pos = jnp.transpose(pos, (0, 2, 1, 3)).reshape(seq_count, rows_here)
    return pos.astype(jnp.float32)


def local(
    query_rows,
    key_rows,
    stored_value_rows,
    output_grad,
    layer_input,
    key_matrix,
    value_matrix,
    run_placement,
):
    seq_index = lax.axis_index("seq")
    seq_count = run_placement.shape[0]
    rows_here = query_rows.shape[0]
    kv_width = key_rows.shape[1]
    features = layer_input.shape[1]
    parts = (key_matrix.shape[0] // features) * (kv_width // HEAD_SIZE)

    def cut(array):
        return array.reshape(parts, rows_here // parts, array.shape[1])

    query_grad, input_grad, key_weight, value_weight = step(
        seq_count,
        cut(query_rows),
        cut(output_grad),
        cut(key_rows),
        cut(stored_value_rows),
        positions(run_placement, rows_here, parts),
        cut(layer_input),
        key_matrix,
        value_matrix,
    )
    query_grad, input_grad, key_weight, value_weight = deliver(
        query_grad, input_grad, key_weight, value_weight
    )
    block_width = 2 * features // seq_count
    if key_weight.shape[0] != block_width:
        shift = (seq_index * block_width) % key_weight.shape[0]
        key_weight = lax.dynamic_slice_in_dim(key_weight, shift, block_width, 0)
        value_weight = lax.dynamic_slice_in_dim(value_weight, shift, block_width, 0)
    return (query_grad.reshape(query_rows.shape), input_grad, key_weight, value_weight)


def solution(mesh):
    placed = (P("seq", "tp"),) * 5 + (P(None, "tp"), P(None, "tp"), P())
    return jax.shard_map(
        local,
        mesh=mesh,
        in_specs=placed,
        out_specs=(P("seq", "tp"),) * 4,
        check_vma=False,
    )
```

```python
import math

import jax
import jax.numpy as jnp
from jax import lax
from jax.experimental import pallas as pl
from jax.experimental.pallas import tpu as pltpu
from jax.sharding import PartitionSpec as P

HEAD_SIZE = 128
WINDOW_LENGTH = 4096
GROUP = 4
CHUNK = 512
MASKED = -1e30
NT = (((1,), (1,)), ((), ()))
NN = (((1,), (0,)), ((), ()))
TN = (((0,), (0,)), ((), ()))
MESH = pl.DeviceIdType.MESH


def dot(a, b, dims):
    return lax.dot_general(a, b, dims, preferred_element_type=jnp.float32)


def flip(index, bit):
    return index + bit - 2 * bit * ((index // bit) % 2)


def visible(parts, keys):
    return [
        (a, b)
        for a in range(parts)
        for b in range(a + 1)
        if (a - b - 1) * keys + 1 < WINDOW_LENGTH
    ]


def step_kernel(
    q_in, g_in, k_in, v_in, place_ref, x_ref, km_ref, vm_ref,
    dq_ref, ig_ref, kw_ref, vw_ref,
    kv_ref, qb_ref, gb_ref, kpos_ref, s_ref, dp_ref, p_ref, ds_ref, dqb_ref, dqa_ref,
    sum_ref, give_ref, take_ref, land_ref, wk_ref, xs_ref, acc_ref,
    own_ref, out_ref, got_ref, near_ref, far_ref, q_ref, g_ref, k_ref, v_ref, pos_ref,
    plane_send, kv_recv, kvz_send, kvp_send, kvp_recv, qg_send, qg_recv,
    x_sent, x_recv, side_send, side_recv, local_sem,
    give_send, give_recv, z_send, z_recv,
    xp_send, xr_recv, xd_send, xd_recv, wk_send, wk_recv, own_sem, share_sem,
    dq_send, dq_recv,
):
    n = lax.axis_size("seq")
    cores = lax.axis_size("tp")
    me = lax.axis_index("seq")
    tp = lax.axis_index("tp")
    parts, run, _ = q_ref.shape
    kv_local = k_ref.shape[2] // HEAD_SIZE
    plane = cores * kv_local
    pair = GROUP // cores
    depth = n // plane
    z = me // plane
    p = me % plane
    home = p // kv_local
    lane = p % kv_local
    block = plane * run
    keys = n * run
    wide = pair * block
    sub = min(keys, CHUNK)
    roomy = dp_ref.shape[0] > 1
    windowed = parts * keys > WINDOW_LENGTH
    features = x_ref.shape[2]
    x_width = xs_ref.shape[2]
    scale = 1.0 / math.sqrt(HEAD_SIZE)
    power = scale * math.log2(math.e)
    other = {"seq": me, "tp": 1 - tp}

    owner = home == tp
    guest = jnp.logical_not(owner)

    def when(cond, action):
        if cond is None:
            action()
        else:
            pl.when(cond)(action)

    def send(src, dst, send_sem, recv_sem, device, cond=None):
        def copy():
            return pltpu.make_async_remote_copy(
                src_ref=src, dst_ref=dst, send_sem=send_sem, recv_sem=recv_sem,
                device_id=device, device_id_type=MESH,
            )

        when(cond, lambda: copy().start())

    def left(src, send_sem, cond=None):
        def wait():
            pltpu.make_async_remote_copy(
                src_ref=src, dst_ref=src, send_sem=send_sem, recv_sem=send_sem,
                device_id=other, device_id_type=MESH,
            ).wait_send()

        when(cond, wait)

    def arrive(dst, recv_sem, cond=None):
        def wait():
            pltpu.make_async_remote_copy(
                src_ref=dst, dst_ref=dst, send_sem=recv_sem, recv_sem=recv_sem,
                device_id=other, device_id_type=MESH,
            ).wait_recv()

        when(cond, wait)

    def rows_of(index, count):
        return pl.ds(pl.multiple_of(index * count, count), count)

    def lanes_of(index):
        return pl.ds(pl.multiple_of(index * HEAD_SIZE, HEAD_SIZE), HEAD_SIZE)

    bits = [1 << e for e in range(depth.bit_length() - 1)]
    order = sorted(range(depth), key=lambda k: (bin(k).count("1"), -k))

    def layer(k):
        index = z
        for bit in bits:
            if k & bit:
                index = flip(index, bit)
        return index

    def lower(k):
        return [bit for bit in reversed(bits) if k == 0 or bit < (k & -k)]

    layers = depth // cores
    holder = tp == z // layers
    flips = ((1,), (2,), (1, 2))

    def block_of(source):
        return xs_ref.at[:, rows_of(source, run), :]

    def columns_of(target):
        start = (target % layers) * x_width
        return x_ref.at[:, :, pl.ds(pl.multiple_of(start, x_width), x_width)]

    staged = []
    for src, dst in ((k_in, k_ref), (v_in, v_ref), (q_in, q_ref), (g_in, g_ref)):
        staged.append(pltpu.make_async_copy(src, dst, local_sem.at[3 + len(staged)]))
        staged[-1].start()

    own_columns = pltpu.make_async_copy(columns_of(z), block_of(me), local_sem.at[2])
    pl.when(holder)(own_columns.start)

    def x_send(slot, early):
        target = tp * layers + (z + layers - 1 - slot) % layers
        clear = (target > z) == (z % 2 == 1)
        now = clear if early else jnp.logical_not(clear)
        send(
            columns_of(target), block_of(me), x_sent, x_recv.at[z],
            {"seq": target * plane + p, "tp": tp}, (target != z) & now,
        )

    def turned(index, ways):
        for bit in ways:
            index = flip(index, bit)
        return index

    def x_push(k):
        block = block_of(layer(k) * plane + p)
        if k == 0:
            pl.when(holder)(own_columns.wait)
        else:
            arrive(block, x_recv.at[layer(k)], holder)
        for way, ways in enumerate(flips):
            send(block, block, xp_send, xr_recv.at[way, k],
                 {"seq": z * plane + turned(p, ways), "tp": tp}, holder)
        send(block, block, xd_send, xd_recv, other, holder)

    def x_relay(k):
        for way, ways in enumerate(flips):
            block = block_of(layer(k) * plane + turned(p, ways))
            arrive(block, xr_recv.at[way, k], holder)
            send(block, block, xd_send, xd_recv, other, holder)

    barrier = pltpu.get_barrier_semaphore()
    for step in range(n):
        for core in range(cores):
            if step or core:
                pl.semaphore_signal(
                    barrier,
                    inc=1,
                    device_id={"seq": (me + step) % n, "tp": (tp + core) % cores},
                    device_id_type=MESH,
                )
    pl.semaphore_wait(barrier, n * cores - 1)

    for copy in staged:
        copy.wait()

    def piece(role, source):
        return kv_ref.at[role, :, rows_of(source, run), :]

    for i in range(kv_local):
        head = tp * kv_local + i
        target = z * plane + head
        for role, ref in enumerate((k_ref, v_ref)):
            mine = (head == p) & (tp == role)
            cols = slice(i * HEAD_SIZE, (i + 1) * HEAD_SIZE)
            send(
                ref.at[:, :, cols], piece(role, me), plane_send.at[i, role], kv_recv.at[me],
                {"seq": target, "tp": role}, jnp.logical_not(mine),
            )

            @pl.when(mine)
            def _():
                kv_ref[role, :, rows_of(me, run), :] = ref[:, :, cols]

    for i in range(kv_local):
        head = tp * kv_local + i
        target = z * plane + head
        for u in range(cores):
            mine = (head == p) & (tp == u)
            for h in range(pair):
                first = (i * GROUP + u * pair + h) * HEAD_SIZE
                cols = slice(first, first + HEAD_SIZE)
                for w, (ref, buf) in enumerate(((q_ref, qb_ref), (g_ref, gb_ref))):
                    send(
                        ref.at[:, :, cols], buf.at[:, h, rows_of(p, run), :],
                        qg_send.at[w], qg_recv.at[w],
                        {"seq": target, "tp": u}, jnp.logical_not(mine),
                    )

                    @pl.when(mine)
                    def _():
                        buf[:, h, rows_of(p, run), :] = ref[:, :, cols]

    x_push(0)

    short = parts * run // n
    count = run // short
    column = lax.broadcasted_iota(jnp.int32, (n, block), 1)
    row = lax.broadcasted_iota(jnp.int32, (n, block), 0)
    slot = column % run // short
    table = place_ref[...].astype(jnp.bfloat16)
    for s in range(depth):
        picks = (row == s * plane + column // run).astype(jnp.bfloat16)
        slots = dot(table, picks, NN)
        for a in range(parts):
            chosen = jnp.where(row == a * count + slot, slots, 0.0)
            start = (a * count + slot[:1]) * (parts * run) + column[:1] % short
            pos_ref[s * parts + a : s * parts + a + 1, :] = (
                jnp.sum(chosen, axis=0, keepdims=True) * short + start.astype(jnp.float32)
            )
    pos_t = jnp.transpose(pos_ref[...])
    for b in range(parts):
        for s in range(depth):
            column = pos_t[:, s * parts + b : s * parts + b + 1]
            kpos_ref[b, s * block : (s + 1) * block, :] = jnp.broadcast_to(column, (block, block))

    def pass_on(k):
        for j in range(plane):
            source = layer(k) * plane + (p + j) % plane
            place = piece(tp, source)
            arrive(place, kv_recv.at[source], home != tp if k + j == 0 else None)
            for bit in lower(k):
                send(place, place, kvz_send, kv_recv.at[source],
                     {"seq": flip(z, bit) * plane + p, "tp": tp})
            send(place, place, kvp_send, kvp_recv, other)

    relayed = [k for k in order if lower(k)]
    pass_on(0)
    for slot in range(layers):
        x_send(slot, True)
    for k in relayed[1:]:
        pass_on(k)

    def half_of(src, core):
        return src.at[pl.ds(pl.multiple_of(core * features, features), features), :]

    nearby = []
    for i, src in enumerate((km_ref, vm_ref)):
        send(half_of(src, 1 - tp), far_ref.at[i], side_send.at[i], side_recv.at[i], other)
        nearby.append(pltpu.make_async_copy(half_of(src, tp), near_ref.at[i], local_sem.at[i]))
        nearby[-1].start()

    for slot in range(layers):
        x_send(slot, False)

    for k in order:
        if k not in relayed:
            pass_on(k)

    fewer = (plane - 1) * run
    for w, buf in enumerate((qb_ref, gb_ref)):
        arrive(buf, qg_recv.at[w], guest)
        arrive(buf.at[:, :, :fewer, :], qg_recv.at[w], owner)
    arrive(kv_ref.at[1 - tp], kvp_recv)

    tiles = visible(parts, keys)

    def lowest(a):
        return min(b for c, b in tiles if c == a)

    where = {tile: t for t, tile in enumerate(tiles)}

    def sweep(body, carry):
        if keys == sub:
            return body(slice(0, keys), carry)
        return lax.fori_loop(0, keys // sub, lambda i, c: body(rows_of(i, sub), c), carry)

    x_relay(0)
    inverse, delta = [], []
    for a in range(parts):
        qa = qb_ref[a].reshape(wide, HEAD_SIZE)
        ga = gb_ref[a].reshape(wide, HEAD_SIZE)
        qpos = pos_ref[pl.ds(z * parts + a, 1), :]
        lows = range(lowest(a), a + 1)
        top = jnp.full((1, wide), MASKED, jnp.float32)
        for b in lows:

            def scores(at, top):
                s = dot(kv_ref[0, b, at, :], qa, NT)
                if a == b or windowed:
                    kpos = kpos_ref[b, at, :]
                    seen = kpos <= qpos
                    if windowed:
                        seen = seen & (kpos > qpos - WINDOW_LENGTH)
                    s = jnp.concatenate(
                        [
                            jnp.where(seen, s[:, h * block : (h + 1) * block], MASKED)
                            for h in range(pair)
                        ],
                        axis=1,
                    )
                s_ref[where[a, b], at, :] = s
                return jnp.maximum(top, jnp.max(s, axis=0, keepdims=True))

            top = sweep(scores, top)
        carry = (jnp.zeros((1, wide), jnp.float32), jnp.zeros((1, wide), jnp.float32))
        for b in lows:

            def sums(at, carry):
                total, weighted = carry
                e = jnp.exp2((s_ref[where[a, b], at, :] - top) * power)
                dp = dot(kv_ref[1, b, at, :], ga, NT)
                s_ref[where[a, b], at, :] = e
                if roomy:
                    dp_ref[where[a, b], at, :] = dp
                return (
                    total + jnp.sum(e, axis=0, keepdims=True),
                    weighted + jnp.sum(e * dp, axis=0, keepdims=True),
                )

            carry = sweep(sums, carry)
        total, weighted = carry
        inverse.append(1.0 / total)
        delta.append(weighted / total)

    def backward(b):
        uppers = [a for a in range(parts) if (a, b) in where]
        lo, hi = uppers[0], uppers[-1] + 1
        d = b if roomy else 0
        for a in uppers:
            lanes = slice(a * wide, (a + 1) * wide)

            def grads(at, carry):
                prob = s_ref[where[a, b], at, :] * inverse[a]
                if roomy:
                    dp = dp_ref[where[a, b], at, :]
                else:
                    dp = dot(kv_ref[1, b, at, :], gb_ref[a].reshape(wide, HEAD_SIZE), NT)
                p_ref[at, lanes] = prob.astype(jnp.bfloat16)
                ds_ref[d, at, lanes] = (prob * (dp - delta[a])).astype(jnp.bfloat16)
                return carry

            sweep(grads, 0)
        lanes = slice(lo * wide, hi * wide)
        q_all = qb_ref[lo:hi].reshape((hi - lo) * wide, HEAD_SIZE)
        g_all = gb_ref[lo:hi].reshape((hi - lo) * wide, HEAD_SIZE)

        def products(at, carry):
            dk = dot(ds_ref[d, at, lanes], q_all, NN) * scale
            dv = dot(p_ref[at, lanes], g_all, NN)
            first = tp == 0
            sum_ref[b, at, :] = jnp.where(first, dk, dv)
            give_ref[b, at, :] = jnp.where(first, dv, dk).astype(jnp.bfloat16)
            return carry

        sweep(products, 0)
        send(give_ref.at[b], take_ref.at[b], give_send, give_recv.at[b], other)
        if not roomy:
            for a in uppers:
                query_sum(a, b)

    def query_sum(a, b):
        d = b if roomy else 0
        lanes = slice(a * wide, (a + 1) * wide)

        def add(at, acc):
            return acc + dot(kv_ref[0, b, at, :], ds_ref[d, at, lanes], TN)

        acc = sweep(add, jnp.zeros((HEAD_SIZE, wide), jnp.float32))
        if b == a:
            dqa_ref[a] = acc
        else:
            dqa_ref[a] += acc

    def exchange(b, e):
        bit = bits[e]
        first = depth - depth // bit
        for t in range(depth // (2 * bit)):
            to = flip(z, bit) % (2 * bit) + t * 2 * bit
            rows = rows_of(to, block)
            take_ref[b, rows, :] = sum_ref[b, rows, :].astype(jnp.bfloat16)
            send(
                take_ref.at[b, rows, :], land_ref.at[b, first + t], z_send,
                z_recv.at[b, e], {"seq": flip(z, bit) * plane + p, "tp": tp},
            )

    def cross(b):
        arrive(take_ref.at[b], give_recv.at[b])
        sum_ref[b] += take_ref[b].astype(jnp.float32)
        exchange(b, 0)

    def add_landed(b, e):
        bit = bits[e]
        count = depth // (2 * bit)
        first = depth - depth // bit
        arrive(land_ref.at[b, first : first + count], z_recv.at[b, e])
        for t in range(count):
            rows = rows_of(z % (2 * bit) + t * 2 * bit, block)
            sum_ref[b, rows, :] += land_ref[b, first + t].astype(jnp.float32)

    def fold(e):
        def go(b):
            add_landed(b, e - 1)
            exchange(b, e)

        return go

    def finish(b):
        add_landed(b, len(bits) - 1)
        rows = rows_of(z, block)
        wk_ref[b, rows, :] = sum_ref[b, rows, :].astype(jnp.bfloat16)
        carry(b, 0)

    def carry(b, k):
        place = wk_ref.at[b, rows_of(layer(k), block), :]
        for bit in lower(k):
            send(place, place, wk_send, wk_recv.at[b, layer(k)],
                 {"seq": flip(z, bit) * plane + p, "tp": tp})

    def collect(b, k):
        arrive(wk_ref.at[b, rows_of(layer(k), block), :], wk_recv.at[b, layer(k)])

    def hand(b):
        for k in relayed[1:]:
            collect(b, k)
            carry(b, k)

    def gather(b):
        for k in order:
            if k not in relayed:
                collect(b, k)

    def weigh(b, first):
        part = dot(wk_ref[b], xs_ref[b], TN)
        if first:
            acc_ref[...] = part
        else:
            acc_ref[...] += part

    def own_send():
        for j in range(plane):
            src = wk_ref.at[:, rows_of(z * plane + j, run), :]
            for core in range(cores):
                mine = (p == j) & (tp == core)
                index = tp * plane + p
                send(src, own_ref.at[index], own_sem.at[0], own_sem.at[1],
                     {"seq": z * plane + j, "tp": core}, jnp.logical_not(mine))

                @pl.when(mine)
                def _():
                    own_ref[index] = wk_ref[:, rows_of(z * plane + j, run), :]

    def share():
        grads = jnp.transpose(acc_ref[...]).astype(jnp.bfloat16)
        rows = grads.shape[0] // plane
        for j in range(plane):
            out_ref[j] = grads[j * rows : (j + 1) * rows]
        for ways in ((1, 2), (1,), (2,), ()):
            j = turned(p, ways)
            send(out_ref.at[j], got_ref.at[tp * kv_local + lane], share_sem.at[0], share_sem.at[1],
                 {"seq": z * plane + j, "tp": home}, None if ways else guest)

        @pl.when(owner)
        def _():
            got_ref[tp * kv_local + lane] = out_ref[p]

    def queries():
        for a in range(parts):
            if roomy:
                for b in reversed(range(lowest(a), a + 1)):
                    query_sum(a, b)
            out = (jnp.transpose(dqa_ref[a]) * scale).astype(jnp.bfloat16)
            dqb_ref[a] = out.reshape(pair, block, HEAD_SIZE)
        for j in range(plane):
            for h in range(pair):
                cols = lanes_of(lane * GROUP + tp * pair + h)
                mine = (p == j) & (home == tp)
                src = dqb_ref.at[:, h, j * run : (j + 1) * run, :]
                send(
                    src, dq_ref.at[:, :, cols], dq_send, dq_recv,
                    {"seq": z * plane + j, "tp": home}, jnp.logical_not(mine),
                )

                @pl.when(mine)
                def _():
                    dq_ref[:, :, cols] = dqb_ref[:, h, j * run : (j + 1) * run, :]

    def answers():
        arrive(dqb_ref, dq_recv, guest)
        arrive(dqb_ref.at[:, :, :fewer, :], dq_recv, owner)

    def inputs():
        for copy in nearby:
            copy.wait()
        for i in range(2):
            arrive(far_ref.at[i], side_recv.at[i])
        arrive(own_ref.at[: cores * plane - 1], own_sem.at[1])
        rows = parts * run
        grads = [
            own_ref[role * plane + core * kv_local + i].reshape(rows, HEAD_SIZE)
            for core in (tp, 1 - tp)
            for role in range(2)
            for i in range(kv_local)
        ]
        grads = jnp.concatenate(grads, axis=1)
        for f in range(0, features, CHUNK):
            tile = slice(f, min(f + CHUNK, features))
            weights = [ref[i, tile, :] for ref in (near_ref, far_ref) for i in range(2)]
            out = dot(grads, jnp.concatenate(weights, axis=1), NT)
            ig_ref[:, tile] = out.astype(jnp.bfloat16)

    last = parts - 1
    for b in reversed(range(parts)):
        backward(b)
        if b < last:
            cross(b + 1)
        if b == last - 1:
            x_push(1)
    cross(0)
    for k in range(2, depth):
        x_push(k)
    stages = [fold(e) for e in range(1, len(bits))] + [finish, hand]
    for tick in range(last + len(stages)):
        for level, stage in enumerate(stages):
            b = last - (tick - level)
            if 0 <= b <= last:
                stage(b)
        if tick == last:
            x_relay(1)
            queries()
        if tick == last + 1:
            x_relay(2)
    for k in range(3, depth):
        x_relay(k)
    own_send()
    arrive(xs_ref, xd_recv, jnp.logical_not(holder))
    for b in reversed(range(parts)):
        gather(b)
        weigh(b, b == last)
    share()
    answers()
    inputs()
    arrive(got_ref, share_sem.at[1], guest)
    arrive(got_ref.at[: cores * kv_local - 1], share_sem.at[1], owner)
    for role, held in enumerate((kw_ref, vw_ref)):
        for i in range(kv_local):
            cols = slice(i * HEAD_SIZE, (i + 1) * HEAD_SIZE)
            held[:, cols] = got_ref[role * kv_local + i].astype(jnp.float32)
    for i in range(kv_local):
        for role in range(cores):
            mine = (tp * kv_local + i == p) & (tp == role)
            left(piece(role, me), plane_send.at[i, role], jnp.logical_not(mine))
    for w, buf in ((0, qb_ref), (1, gb_ref)):
        left(buf, qg_send.at[w], guest)
        left(buf.at[:, :, :fewer, :], qg_send.at[w], owner)
    moves = sum(len(lower(k)) for k in order)
    left(kv_ref.at[0, :, : moves * block, :], kvz_send)
    left(kv_ref.at[0], kvp_send)
    left(xs_ref.at[:, : layers * run, :], x_sent, jnp.logical_not(holder))
    left(xs_ref.at[:, : (layers - 1) * run, :], x_sent, holder)
    left(xs_ref.at[:, : len(flips) * depth * run, :], xp_send, holder)
    left(xs_ref, xd_send, holder)
    for i in range(2):
        left(far_ref.at[i], side_send.at[i])
    left(give_ref, give_send)
    left(take_ref.at[:, : (depth - 1) * block, :], z_send)
    left(dqb_ref, dq_send, guest)
    left(dqb_ref.at[:, :, :fewer, :], dq_send, owner)
    left(wk_ref.at[:, : moves * block, :], wk_send)
    left(own_ref.at[: cores * plane - 1], own_sem.at[0])
    left(out_ref, share_sem.at[0], guest)
    left(out_ref.at[: plane - 1], share_sem.at[0], owner)


def deliver_kernel(*refs):
    count = (len(refs) - 1) // 2
    moves = []
    for i in range(count):
        moves.append(pltpu.make_async_copy(refs[i], refs[count + i], refs[-1].at[i]))
        moves[-1].start()
    for move in moves:
        move.wait()


def deliver(*arrays):
    vmem = pl.BlockSpec(memory_space=pltpu.VMEM)
    hbm = pl.BlockSpec(memory_space=pl.ANY)
    count = len(arrays)
    return pl.pallas_call(
        deliver_kernel,
        out_shape=tuple(jax.ShapeDtypeStruct(a.shape, a.dtype) for a in arrays),
        in_specs=[vmem] * count,
        out_specs=(hbm,) * count,
        scratch_shapes=[pltpu.SemaphoreType.DMA((count,))],
    )(*arrays)


def step(n, q, g, k, v, place, x, km, vm):
    parts, run, width = q.shape
    kv_width = k.shape[2]
    kv_local = kv_width // HEAD_SIZE
    features = x.shape[2]
    heads = width // HEAD_SIZE
    cores = km.shape[0] // features
    plane = cores * kv_local
    pair = GROUP // cores
    depth = n // plane
    levels = depth.bit_length() - 1
    block = plane * run
    keys = n * run
    wide = pair * block
    block_width = cores * features // n
    x_width = plane * block_width
    roomy = parts * keys <= 4096
    tiles = len(visible(parts, keys))
    vmem = pl.BlockSpec(memory_space=pltpu.VMEM)
    hbm = pl.BlockSpec(memory_space=pl.ANY)
    kind = jnp.bfloat16
    real = jnp.float32
    dma = pltpu.SemaphoreType.DMA
    return pl.pallas_call(
        step_kernel,
        out_shape=(
            jax.ShapeDtypeStruct((parts, run, width), kind),
            jax.ShapeDtypeStruct((parts * run, features), kind),
            jax.ShapeDtypeStruct((block_width, kv_width), real),
            jax.ShapeDtypeStruct((block_width, kv_width), real),
        ),
        in_specs=[hbm] * 4 + [vmem] + [hbm] * 3,
        out_specs=(vmem,) * 4,
        scratch_shapes=[
            pltpu.VMEM((2, parts, keys, HEAD_SIZE), kind),
            pltpu.VMEM((parts, pair, block, HEAD_SIZE), kind),
            pltpu.VMEM((parts, pair, block, HEAD_SIZE), kind),
            pltpu.VMEM((parts, keys, block), real),
            pltpu.VMEM((tiles, keys, wide), real),
            pltpu.VMEM((tiles, keys, wide) if roomy else (1, 8, 128), real),
            pltpu.VMEM((keys, parts * wide), kind),
            pltpu.VMEM((parts if roomy else 1, keys, parts * wide), kind),
            pltpu.VMEM((parts, pair, block, HEAD_SIZE), kind),
            pltpu.VMEM((parts, HEAD_SIZE, wide), real),
            pltpu.VMEM((parts, keys, HEAD_SIZE), real),
            pltpu.VMEM((parts, keys, HEAD_SIZE), kind),
            pltpu.VMEM((parts, keys, HEAD_SIZE), kind),
            pltpu.VMEM((parts, depth - 1, block, HEAD_SIZE), kind),
            pltpu.VMEM((parts, keys, HEAD_SIZE), kind),
            pltpu.VMEM((parts, keys, x_width), kind),
            pltpu.VMEM((HEAD_SIZE, x_width), real),
            pltpu.VMEM((cores * plane, parts, run, HEAD_SIZE), kind),
            pltpu.VMEM((plane, block_width, HEAD_SIZE), kind),
            pltpu.VMEM((cores * kv_local, block_width, HEAD_SIZE), kind),
            pltpu.VMEM((2, features, kv_width), kind),
            pltpu.VMEM((2, features, kv_width), kind),
            pltpu.VMEM((parts, run, width), kind),
            pltpu.VMEM((parts, run, width), kind),
            pltpu.VMEM((parts, run, kv_width), kind),
            pltpu.VMEM((parts, run, kv_width), kind),
            pltpu.VMEM((depth * parts, block), real),
            dma((kv_local, cores)),
            dma((n,)),
            dma,
            dma,
            dma,
            dma((2,)),
            dma((2,)),
            dma,
            dma((depth,)),
            dma((2,)),
            dma((2,)),
            dma((7,)),
            dma,
            dma((parts,)),
            dma,
            dma((parts, levels)),
            dma,
            dma((3, depth)),
            dma,
            dma,
            dma,
            dma((parts, depth)),
            dma((2,)),
            dma((2,)),
            dma,
            dma,
        ],
        compiler_params=pltpu.CompilerParams(
            vmem_limit_bytes=63 * 2**20, collective_id=0, has_side_effects=True
        ),
    )(q, g, k, v, place, x, km, vm)


def local(
    query_rows,
    key_rows,
    stored_value_rows,
    output_grad,
    layer_input,
    key_matrix,
    value_matrix,
    run_placement,
):
    seq_index = lax.axis_index("seq")
    seq_count = run_placement.shape[0]
    rows_here = query_rows.shape[0]
    kv_width = key_rows.shape[1]
    parts = (key_matrix.shape[0] // layer_input.shape[1]) * (kv_width // HEAD_SIZE)

    def cut(array):
        return array.reshape(parts, rows_here // parts, array.shape[1])

    query_grad, input_grad, key_weight, value_weight = step(
        seq_count,
        cut(query_rows),
        cut(output_grad),
        cut(key_rows),
        cut(stored_value_rows),
        run_placement,
        cut(layer_input),
        key_matrix,
        value_matrix,
    )
    query_grad, input_grad, key_weight, value_weight = deliver(
        query_grad, input_grad, key_weight, value_weight
    )
    return (query_grad.reshape(query_rows.shape), input_grad, key_weight, value_weight)


def solution(mesh):
    placed = (P("seq", "tp"),) * 5 + (P(None, "tp"), P(None, "tp"), P())
    return jax.shard_map(
        local,
        mesh=mesh,
        in_specs=placed,
        out_specs=(P("seq", "tp"),) * 4,
        check_vma=False,
    )
```

```python
import math

import jax
import jax.numpy as jnp
from jax import lax
from jax.experimental import pallas as pl
from jax.experimental.pallas import tpu as pltpu
from jax.sharding import PartitionSpec as P

HEAD_SIZE = 128
WINDOW_LENGTH = 4096
GROUP = 4
CHUNK = 512
MASKED = -1e30
NT = (((1,), (1,)), ((), ()))
NN = (((1,), (0,)), ((), ()))
TN = (((0,), (0,)), ((), ()))
MESH = pl.DeviceIdType.MESH


def dot(a, b, dims):
    return lax.dot_general(a, b, dims, preferred_element_type=jnp.float32)


def flip(index, bit):
    return index + bit - 2 * bit * ((index // bit) % 2)


def visible(parts, keys):
    return [
        (a, b)
        for a in range(parts)
        for b in range(a + 1)
        if (a - b - 1) * keys + 1 < WINDOW_LENGTH
    ]


def step_kernel(
    q_in, g_in, k_in, v_in, place_ref, x_ref, km_ref, vm_ref,
    dq_out, ig_out, kw_out, vw_out,
    kv_ref, qb_ref, gb_ref, kpos_ref, s_ref, dp_ref, p_ref, ds_ref, dqb_ref, dqa_ref,
    sum_ref, give_ref, take_ref, land_ref, wk_ref, xs_ref, acc_ref,
    own_ref, out_ref, got_ref, near_ref, far_ref, dq_ref, ig_ref, kw_ref, vw_ref, q_ref, g_ref, k_ref, v_ref, pos_ref,
    plane_send, kv_recv, kvz_send, kvp_send, kvp_recv, qg_send, qg_recv,
    x_sent, x_recv, side_send, side_recv, local_sem,
    give_send, give_recv, z_send, z_recv,
    xp_send, xr_recv, xd_send, xd_recv, wk_send, wk_recv, own_sem, share_sem,
    dq_send, dq_recv,
):
    n = lax.axis_size("seq")
    cores = lax.axis_size("tp")
    me = lax.axis_index("seq")
    tp = lax.axis_index("tp")
    parts, run, _ = q_ref.shape
    kv_local = k_ref.shape[2] // HEAD_SIZE
    plane = cores * kv_local
    pair = GROUP // cores
    depth = n // plane
    z = me // plane
    p = me % plane
    home = p // kv_local
    lane = p % kv_local
    block = plane * run
    keys = n * run
    wide = pair * block
    sub = min(keys, CHUNK)
    roomy = dp_ref.shape[0] > 1
    windowed = parts * keys > WINDOW_LENGTH
    features = x_ref.shape[2]
    x_width = xs_ref.shape[2]
    scale = 1.0 / math.sqrt(HEAD_SIZE)
    power = scale * math.log2(math.e)
    other = {"seq": me, "tp": 1 - tp}

    owner = home == tp
    guest = jnp.logical_not(owner)

    def when(cond, action):
        if cond is None:
            action()
        else:
            pl.when(cond)(action)

    def send(src, dst, send_sem, recv_sem, device, cond=None):
        def copy():
            return pltpu.make_async_remote_copy(
                src_ref=src, dst_ref=dst, send_sem=send_sem, recv_sem=recv_sem,
                device_id=device, device_id_type=MESH,
            )

        when(cond, lambda: copy().start())

    def left(src, send_sem, cond=None):
        def wait():
            pltpu.make_async_remote_copy(
                src_ref=src, dst_ref=src, send_sem=send_sem, recv_sem=send_sem,
                device_id=other, device_id_type=MESH,
            ).wait_send()

        when(cond, wait)

    def arrive(dst, recv_sem, cond=None):
        def wait():
            pltpu.make_async_remote_copy(
                src_ref=dst, dst_ref=dst, send_sem=recv_sem, recv_sem=recv_sem,
                device_id=other, device_id_type=MESH,
            ).wait_recv()

        when(cond, wait)

    def rows_of(index, count):
        return pl.ds(pl.multiple_of(index * count, count), count)

    def lanes_of(index):
        return pl.ds(pl.multiple_of(index * HEAD_SIZE, HEAD_SIZE), HEAD_SIZE)

    bits = [1 << e for e in range(depth.bit_length() - 1)]
    order = sorted(range(depth), key=lambda k: (bin(k).count("1"), -k))

    def layer(k):
        index = z
        for bit in bits:
            if k & bit:
                index = flip(index, bit)
        return index

    def lower(k):
        return [bit for bit in reversed(bits) if k == 0 or bit < (k & -k)]

    layers = depth // cores
    holder = tp == z // layers
    flips = ((1,), (2,), (1, 2))

    def block_of(source):
        return xs_ref.at[:, rows_of(source, run), :]

    def columns_of(target):
        start = (target % layers) * x_width
        return x_ref.at[:, :, pl.ds(pl.multiple_of(start, x_width), x_width)]

    staged = []
    for src, dst in ((k_in, k_ref), (v_in, v_ref), (q_in, q_ref), (g_in, g_ref)):
        staged.append(pltpu.make_async_copy(src, dst, local_sem.at[3 + len(staged)]))
        staged[-1].start()

    own_columns = pltpu.make_async_copy(columns_of(z), block_of(me), local_sem.at[2])
    pl.when(holder)(own_columns.start)

    def x_send(slot, phase):
        target = jnp.where(tp == 0, layers - 1 - slot, tp * layers + slot)
        clear = (target > z) == (z % 2 == 1)
        outer = ((target == 0) | (target == depth - 1)) & (jnp.abs(target - z) > 1)
        now = outer
        if phase < 2:
            now = jnp.logical_not(outer) & (clear if phase == 0 else jnp.logical_not(clear))
        send(
            columns_of(target), block_of(me), x_sent, x_recv.at[z],
            {"seq": target * plane + p, "tp": tp}, (target != z) & now,
        )

    def turned(index, ways):
        for bit in ways:
            index = flip(index, bit)
        return index

    def x_push(k):
        block = block_of(layer(k) * plane + p)
        if k == 0:
            pl.when(holder)(own_columns.wait)
        else:
            arrive(block, x_recv.at[layer(k)], holder)
        for way, ways in enumerate(flips):
            send(block, block, xp_send, xr_recv.at[way, k],
                 {"seq": z * plane + turned(p, ways), "tp": tp}, holder)
        send(block, block, xd_send, xd_recv, other, holder)

    def x_relay(k):
        for way, ways in enumerate(flips):
            block = block_of(layer(k) * plane + turned(p, ways))
            arrive(block, xr_recv.at[way, k], holder)
            send(block, block, xd_send, xd_recv, other, holder)

    barrier = pltpu.get_barrier_semaphore()
    for step in range(n):
        for core in range(cores):
            if step or core:
                pl.semaphore_signal(
                    barrier,
                    inc=1,
                    device_id={"seq": (me + step) % n, "tp": (tp + core) % cores},
                    device_id_type=MESH,
                )
    pl.semaphore_wait(barrier, n * cores - 1)

    for copy in staged:
        copy.wait()

    def piece(role, source):
        return kv_ref.at[role, :, rows_of(source, run), :]

    for i in range(kv_local):
        head = tp * kv_local + i
        target = z * plane + head
        for role, ref in enumerate((k_ref, v_ref)):
            mine = (head == p) & (tp == role)
            cols = slice(i * HEAD_SIZE, (i + 1) * HEAD_SIZE)
            send(
                ref.at[:, :, cols], piece(role, me), plane_send.at[i, role], kv_recv.at[me],
                {"seq": target, "tp": role}, jnp.logical_not(mine),
            )

            @pl.when(mine)
            def _():
                kv_ref[role, :, rows_of(me, run), :] = ref[:, :, cols]

    for i in range(kv_local):
        head = tp * kv_local + i
        target = z * plane + head
        for u in range(cores):
            mine = (head == p) & (tp == u)
            for h in range(pair):
                first = (i * GROUP + u * pair + h) * HEAD_SIZE
                cols = slice(first, first + HEAD_SIZE)
                for w, (ref, buf) in enumerate(((q_ref, qb_ref), (g_ref, gb_ref))):
                    send(
                        ref.at[:, :, cols], buf.at[:, h, rows_of(p, run), :],
                        qg_send.at[w], qg_recv.at[w],
                        {"seq": target, "tp": u}, jnp.logical_not(mine),
                    )

                    @pl.when(mine)
                    def _():
                        buf[:, h, rows_of(p, run), :] = ref[:, :, cols]

    x_push(0)

    short = parts * run // n
    count = run // short
    column = lax.broadcasted_iota(jnp.int32, (n, block), 1)
    row = lax.broadcasted_iota(jnp.int32, (n, block), 0)
    slot = column % run // short
    table = place_ref[...].astype(jnp.bfloat16)
    for s in range(depth):
        picks = (row == s * plane + column // run).astype(jnp.bfloat16)
        slots = dot(table, picks, NN)
        for a in range(parts):
            chosen = jnp.where(row == a * count + slot, slots, 0.0)
            start = (a * count + slot[:1]) * (parts * run) + column[:1] % short
            pos_ref[s * parts + a : s * parts + a + 1, :] = (
                jnp.sum(chosen, axis=0, keepdims=True) * short + start.astype(jnp.float32)
            )
    pos_t = jnp.transpose(pos_ref[...])
    for b in range(parts):
        for s in range(depth):
            column = pos_t[:, s * parts + b : s * parts + b + 1]
            kpos_ref[b, s * block : (s + 1) * block, :] = jnp.broadcast_to(column, (block, block))

    def pass_on(k):
        for j in range(plane):
            source = layer(k) * plane + (p + j) % plane
            place = piece(tp, source)
            arrive(place, kv_recv.at[source], home != tp if k + j == 0 else None)
            for bit in lower(k):
                send(place, place, kvz_send, kv_recv.at[source],
                     {"seq": flip(z, bit) * plane + p, "tp": tp})
            send(place, place, kvp_send, kvp_recv, other)

    relayed = [k for k in order if lower(k)]
    pass_on(0)
    for slot in range(layers):
        x_send(slot, 0)
    for k in relayed[1:]:
        pass_on(k)

    def half_of(src, core):
        return src.at[pl.ds(pl.multiple_of(core * features, features), features), :]

    nearby = []
    for i, src in enumerate((km_ref, vm_ref)):
        send(half_of(src, 1 - tp), far_ref.at[i], side_send.at[i], side_recv.at[i], other)
        nearby.append(pltpu.make_async_copy(half_of(src, tp), near_ref.at[i], local_sem.at[i]))
        nearby[-1].start()

    for slot in range(layers):
        x_send(slot, 1)

    for k in order:
        if k not in relayed:
            pass_on(k)

    fewer = (plane - 1) * run
    for w, buf in enumerate((qb_ref, gb_ref)):
        arrive(buf, qg_recv.at[w], guest)
        arrive(buf.at[:, :, :fewer, :], qg_recv.at[w], owner)
    arrive(kv_ref.at[1 - tp], kvp_recv)

    tiles = visible(parts, keys)

    def lowest(a):
        return min(b for c, b in tiles if c == a)

    where = {tile: t for t, tile in enumerate(tiles)}

    def sweep(body, carry):
        if keys == sub:
            return body(slice(0, keys), carry)
        return lax.fori_loop(0, keys // sub, lambda i, c: body(rows_of(i, sub), c), carry)

    for slot in range(layers):
        x_send(slot, 2)
    x_relay(0)
    inverse, delta = [], []
    for a in range(parts):
        qa = qb_ref[a].reshape(wide, HEAD_SIZE)
        ga = gb_ref[a].reshape(wide, HEAD_SIZE)
        qpos = pos_ref[pl.ds(z * parts + a, 1), :]
        lows = range(lowest(a), a + 1)
        top = jnp.full((1, wide), MASKED, jnp.float32)
        for b in lows:

            def scores(at, top):
                s = dot(kv_ref[0, b, at, :], qa, NT)
                if a == b or windowed:
                    kpos = kpos_ref[b, at, :]
                    seen = kpos <= qpos
                    if windowed:
                        seen = seen & (kpos > qpos - WINDOW_LENGTH)
                    s = jnp.concatenate(
                        [
                            jnp.where(seen, s[:, h * block : (h + 1) * block], MASKED)
                            for h in range(pair)
                        ],
                        axis=1,
                    )
                s_ref[where[a, b], at, :] = s
                return jnp.maximum(top, jnp.max(s, axis=0, keepdims=True))

            top = sweep(scores, top)
        carry = (jnp.zeros((1, wide), jnp.float32), jnp.zeros((1, wide), jnp.float32))
        for b in lows:

            def sums(at, carry):
                total, weighted = carry
                e = jnp.exp2((s_ref[where[a, b], at, :] - top) * power)
                dp = dot(kv_ref[1, b, at, :], ga, NT)
                s_ref[where[a, b], at, :] = e
                if roomy:
                    dp_ref[where[a, b], at, :] = dp
                return (
                    total + jnp.sum(e, axis=0, keepdims=True),
                    weighted + jnp.sum(e * dp, axis=0, keepdims=True),
                )

            carry = sweep(sums, carry)
        total, weighted = carry
        inverse.append(1.0 / total)
        delta.append(weighted / total)

    def backward(b):
        uppers = [a for a in range(parts) if (a, b) in where]
        lo, hi = uppers[0], uppers[-1] + 1
        d = b if roomy else 0
        for a in uppers:
            lanes = slice(a * wide, (a + 1) * wide)

            def grads(at, carry):
                prob = s_ref[where[a, b], at, :] * inverse[a]
                if roomy:
                    dp = dp_ref[where[a, b], at, :]
                else:
                    dp = dot(kv_ref[1, b, at, :], gb_ref[a].reshape(wide, HEAD_SIZE), NT)
                p_ref[at, lanes] = prob.astype(jnp.bfloat16)
                ds_ref[d, at, lanes] = (prob * (dp - delta[a])).astype(jnp.bfloat16)
                return carry

            sweep(grads, 0)
        lanes = slice(lo * wide, hi * wide)
        q_all = qb_ref[lo:hi].reshape((hi - lo) * wide, HEAD_SIZE)
        g_all = gb_ref[lo:hi].reshape((hi - lo) * wide, HEAD_SIZE)

        def products(at, carry):
            dk = dot(ds_ref[d, at, lanes], q_all, NN) * scale
            dv = dot(p_ref[at, lanes], g_all, NN)
            first = tp == 0
            sum_ref[b, at, :] = jnp.where(first, dk, dv)
            give_ref[b, at, :] = jnp.where(first, dv, dk).astype(jnp.bfloat16)
            return carry

        sweep(products, 0)
        send(give_ref.at[b], take_ref.at[b], give_send, give_recv.at[b], other)
        if not roomy:
            for a in uppers:
                query_sum(a, b)

    def query_sum(a, b):
        d = b if roomy else 0
        lanes = slice(a * wide, (a + 1) * wide)

        def add(at, acc):
            return acc + dot(kv_ref[0, b, at, :], ds_ref[d, at, lanes], TN)

        acc = sweep(add, jnp.zeros((HEAD_SIZE, wide), jnp.float32))
        if b == a:
            dqa_ref[a] = acc
        else:
            dqa_ref[a] += acc

    def exchange(b, e):
        bit = bits[e]
        first = depth - depth // bit
        for t in range(depth // (2 * bit)):
            to = flip(z, bit) % (2 * bit) + t * 2 * bit
            rows = rows_of(to, block)
            take_ref[b, rows, :] = sum_ref[b, rows, :].astype(jnp.bfloat16)
            send(
                take_ref.at[b, rows, :], land_ref.at[b, first + t], z_send,
                z_recv.at[b, e], {"seq": flip(z, bit) * plane + p, "tp": tp},
            )

    def cross(b):
        arrive(take_ref.at[b], give_recv.at[b])
        sum_ref[b] += take_ref[b].astype(jnp.float32)
        exchange(b, 0)

    def add_landed(b, e):
        bit = bits[e]
        count = depth // (2 * bit)
        first = depth - depth // bit
        arrive(land_ref.at[b, first : first + count], z_recv.at[b, e])
        for t in range(count):
            rows = rows_of(z % (2 * bit) + t * 2 * bit, block)
            sum_ref[b, rows, :] += land_ref[b, first + t].astype(jnp.float32)

    def fold(e):
        def go(b):
            add_landed(b, e - 1)
            exchange(b, e)

        return go

    def finish(b):
        add_landed(b, len(bits) - 1)
        rows = rows_of(z, block)
        wk_ref[b, rows, :] = sum_ref[b, rows, :].astype(jnp.bfloat16)
        carry(b, 0)

    def carry(b, k):
        place = wk_ref.at[b, rows_of(layer(k), block), :]
        for bit in lower(k):
            send(place, place, wk_send, wk_recv.at[b, layer(k)],
                 {"seq": flip(z, bit) * plane + p, "tp": tp})

    def collect(b, k):
        arrive(wk_ref.at[b, rows_of(layer(k), block), :], wk_recv.at[b, layer(k)])

    def hand(b):
        for k in relayed[1:]:
            collect(b, k)
            carry(b, k)

    def gather(b):
        for k in order:
            if k not in relayed:
                collect(b, k)

    def weigh(b, first):
        part = dot(wk_ref[b], xs_ref[b], TN)
        if first:
            acc_ref[...] = part
        else:
            acc_ref[...] += part

    def own_send():
        for j in range(plane):
            src = wk_ref.at[:, rows_of(z * plane + j, run), :]
            for core in range(cores):
                mine = (p == j) & (tp == core)
                index = tp * plane + p
                send(src, own_ref.at[index], own_sem.at[0], own_sem.at[1],
                     {"seq": z * plane + j, "tp": core}, jnp.logical_not(mine))

                @pl.when(mine)
                def _():
                    own_ref[index] = wk_ref[:, rows_of(z * plane + j, run), :]

    def share():
        grads = jnp.transpose(acc_ref[...]).astype(jnp.bfloat16)
        rows = grads.shape[0] // plane
        for j in range(plane):
            out_ref[j] = grads[j * rows : (j + 1) * rows]
        for ways in ((1, 2), (1,), (2,), ()):
            j = turned(p, ways)
            send(out_ref.at[j], got_ref.at[tp * kv_local + lane], share_sem.at[0], share_sem.at[1],
                 {"seq": z * plane + j, "tp": home}, None if ways else guest)

        @pl.when(owner)
        def _():
            got_ref[tp * kv_local + lane] = out_ref[p]

    def queries():
        for a in range(parts):
            if roomy:
                for b in reversed(range(lowest(a), a + 1)):
                    query_sum(a, b)
            out = (jnp.transpose(dqa_ref[a]) * scale).astype(jnp.bfloat16)
            dqb_ref[a] = out.reshape(pair, block, HEAD_SIZE)
        for j in range(plane):
            for h in range(pair):
                cols = lanes_of(lane * GROUP + tp * pair + h)
                mine = (p == j) & (home == tp)
                src = dqb_ref.at[:, h, j * run : (j + 1) * run, :]
                send(
                    src, dq_ref.at[:, :, cols], dq_send, dq_recv,
                    {"seq": z * plane + j, "tp": home}, jnp.logical_not(mine),
                )

                @pl.when(mine)
                def _():
                    dq_ref[:, :, cols] = dqb_ref[:, h, j * run : (j + 1) * run, :]

    leaving = []

    def put(src, dst):
        leaving.append(pltpu.make_async_copy(src, dst, local_sem.at[7 + len(leaving)]))
        leaving[-1].start()

    def answers():
        arrive(dqb_ref, dq_recv, guest)
        arrive(dqb_ref.at[:, :, :fewer, :], dq_recv, owner)
        put(dq_ref, dq_out)

    def inputs():
        for copy in nearby:
            copy.wait()
        for i in range(2):
            arrive(far_ref.at[i], side_recv.at[i])
        arrive(own_ref.at[: cores * plane - 1], own_sem.at[1])
        rows = parts * run
        grads = [
            own_ref[role * plane + core * kv_local + i].reshape(rows, HEAD_SIZE)
            for core in (tp, 1 - tp)
            for role in range(2)
            for i in range(kv_local)
        ]
        grads = jnp.concatenate(grads, axis=1)
        for f in range(0, features, CHUNK):
            tile = slice(f, min(f + CHUNK, features))
            weights = [ref[i, tile, :] for ref in (near_ref, far_ref) for i in range(2)]
            out = dot(grads, jnp.concatenate(weights, axis=1), NT)
            ig_ref[:, tile] = out.astype(jnp.bfloat16)
        put(ig_ref, ig_out)

    last = parts - 1
    for b in reversed(range(parts)):
        backward(b)
        if b < last:
            cross(b + 1)
        if b == last - 1:
            x_push(1)
    cross(0)
    for k in range(2, depth):
        x_push(k)
    stages = [fold(e) for e in range(1, len(bits))] + [finish, hand]
    for tick in range(last + len(stages)):
        for level, stage in enumerate(stages):
            b = last - (tick - level)
            if 0 <= b <= last:
                stage(b)
        if tick == last:
            x_relay(1)
        if tick == last + len(stages) - 2:
            own_send()
            for k in range(2, depth):
                x_relay(k)
            queries()
    arrive(xs_ref, xd_recv, jnp.logical_not(holder))
    for b in reversed(range(parts)):
        gather(b)
        weigh(b, b == last)
    share()
    inputs()
    answers()
    arrive(got_ref, share_sem.at[1], guest)
    arrive(got_ref.at[: cores * kv_local - 1], share_sem.at[1], owner)
    for role, (held, out) in enumerate(((kw_ref, kw_out), (vw_ref, vw_out))):
        for i in range(kv_local):
            cols = slice(i * HEAD_SIZE, (i + 1) * HEAD_SIZE)
            held[:, cols] = got_ref[role * kv_local + i].astype(jnp.float32)
        put(held, out)
    for i in range(kv_local):
        for role in range(cores):
            mine = (tp * kv_local + i == p) & (tp == role)
            left(piece(role, me), plane_send.at[i, role], jnp.logical_not(mine))
    for w, buf in ((0, qb_ref), (1, gb_ref)):
        left(buf, qg_send.at[w], guest)
        left(buf.at[:, :, :fewer, :], qg_send.at[w], owner)
    moves = sum(len(lower(k)) for k in order)
    left(kv_ref.at[0, :, : moves * block, :], kvz_send)
    left(kv_ref.at[0], kvp_send)
    left(xs_ref.at[:, : layers * run, :], x_sent, jnp.logical_not(holder))
    left(xs_ref.at[:, : (layers - 1) * run, :], x_sent, holder)
    left(xs_ref.at[:, : len(flips) * depth * run, :], xp_send, holder)
    left(xs_ref, xd_send, holder)
    for i in range(2):
        left(far_ref.at[i], side_send.at[i])
    left(give_ref, give_send)
    left(take_ref.at[:, : (depth - 1) * block, :], z_send)
    left(dqb_ref, dq_send, guest)
    left(dqb_ref.at[:, :, :fewer, :], dq_send, owner)
    left(wk_ref.at[:, : moves * block, :], wk_send)
    left(own_ref.at[: cores * plane - 1], own_sem.at[0])
    left(out_ref, share_sem.at[0], guest)
    left(out_ref.at[: plane - 1], share_sem.at[0], owner)
    for copy in leaving:
        copy.wait()


def deliver_kernel(*refs):
    count = (len(refs) - 1) // 3
    ins, outs, held = refs[:count], refs[count : 2 * count], refs[2 * count : 3 * count]
    moves = []
    for i in range(count):
        moves.append(pltpu.make_async_copy(ins[i], held[i], refs[-1].at[0, i]))
        moves[-1].start()
    for i in range(count):
        moves[i].wait()
        moves.append(pltpu.make_async_copy(held[i], outs[i], refs[-1].at[1, i]))
        moves[-1].start()
    for move in moves[count:]:
        move.wait()


def deliver(*arrays):
    hbm = pl.BlockSpec(memory_space=pl.ANY)
    count = len(arrays)
    return pl.pallas_call(
        deliver_kernel,
        out_shape=tuple(jax.ShapeDtypeStruct(a.shape, a.dtype) for a in arrays),
        in_specs=[hbm] * count,
        out_specs=(hbm,) * count,
        scratch_shapes=[pltpu.VMEM(a.shape, a.dtype) for a in arrays]
        + [pltpu.SemaphoreType.DMA((2, count))],
    )(*arrays)


def step(n, q, g, k, v, place, x, km, vm):
    parts, run, width = q.shape
    kv_width = k.shape[2]
    kv_local = kv_width // HEAD_SIZE
    features = x.shape[2]
    heads = width // HEAD_SIZE
    cores = km.shape[0] // features
    plane = cores * kv_local
    pair = GROUP // cores
    depth = n // plane
    levels = depth.bit_length() - 1
    block = plane * run
    keys = n * run
    wide = pair * block
    block_width = cores * features // n
    x_width = plane * block_width
    roomy = parts * keys <= 4096
    tiles = len(visible(parts, keys))
    vmem = pl.BlockSpec(memory_space=pltpu.VMEM)
    hbm = pl.BlockSpec(memory_space=pl.ANY)
    kind = jnp.bfloat16
    real = jnp.float32
    dma = pltpu.SemaphoreType.DMA
    return pl.pallas_call(
        step_kernel,
        out_shape=(
            jax.ShapeDtypeStruct((parts, run, width), kind),
            jax.ShapeDtypeStruct((parts * run, features), kind),
            jax.ShapeDtypeStruct((block_width, kv_width), real),
            jax.ShapeDtypeStruct((block_width, kv_width), real),
        ),
        in_specs=[hbm] * 4 + [vmem] + [hbm] * 3,
        out_specs=(hbm,) * 4,
        scratch_shapes=[
            pltpu.VMEM((2, parts, keys, HEAD_SIZE), kind),
            pltpu.VMEM((parts, pair, block, HEAD_SIZE), kind),
            pltpu.VMEM((parts, pair, block, HEAD_SIZE), kind),
            pltpu.VMEM((parts, keys, block), real),
            pltpu.VMEM((tiles, keys, wide), real),
            pltpu.VMEM((tiles, keys, wide) if roomy else (1, 8, 128), real),
            pltpu.VMEM((keys, parts * wide), kind),
            pltpu.VMEM((parts if roomy else 1, keys, parts * wide), kind),
            pltpu.VMEM((parts, pair, block, HEAD_SIZE), kind),
            pltpu.VMEM((parts, HEAD_SIZE, wide), real),
            pltpu.VMEM((parts, keys, HEAD_SIZE), real),
            pltpu.VMEM((parts, keys, HEAD_SIZE), kind),
            pltpu.VMEM((parts, keys, HEAD_SIZE), kind),
            pltpu.VMEM((parts, depth - 1, block, HEAD_SIZE), kind),
            pltpu.VMEM((parts, keys, HEAD_SIZE), kind),
            pltpu.VMEM((parts, keys, x_width), kind),
            pltpu.VMEM((HEAD_SIZE, x_width), real),
            pltpu.VMEM((cores * plane, parts, run, HEAD_SIZE), kind),
            pltpu.VMEM((plane, block_width, HEAD_SIZE), kind),
            pltpu.VMEM((cores * kv_local, block_width, HEAD_SIZE), kind),
            pltpu.VMEM((2, features, kv_width), kind),
            pltpu.VMEM((2, features, kv_width), kind),
            pltpu.VMEM((parts, run, width), kind),
            pltpu.VMEM((parts * run, features), kind),
            pltpu.VMEM((block_width, kv_width), real),
            pltpu.VMEM((block_width, kv_width), real),
            pltpu.VMEM((parts, run, width), kind),
            pltpu.VMEM((parts, run, width), kind),
            pltpu.VMEM((parts, run, kv_width), kind),
            pltpu.VMEM((parts, run, kv_width), kind),
            pltpu.VMEM((depth * parts, block), real),
            dma((kv_local, cores)),
            dma((n,)),
            dma,
            dma,
            dma,
            dma((2,)),
            dma((2,)),
            dma,
            dma((depth,)),
            dma((2,)),
            dma((2,)),
            dma((11,)),
            dma,
            dma((parts,)),
            dma,
            dma((parts, levels)),
            dma,
            dma((3, depth)),
            dma,
            dma,
            dma,
            dma((parts, depth)),
            dma((2,)),
            dma((2,)),
            dma,
            dma,
        ],
        compiler_params=pltpu.CompilerParams(
            vmem_limit_bytes=63 * 2**20, collective_id=0, has_side_effects=True
        ),
    )(q, g, k, v, place, x, km, vm)


def local(
    query_rows,
    key_rows,
    stored_value_rows,
    output_grad,
    layer_input,
    key_matrix,
    value_matrix,
    run_placement,
):
    seq_index = lax.axis_index("seq")
    seq_count = run_placement.shape[0]
    rows_here = query_rows.shape[0]
    kv_width = key_rows.shape[1]
    parts = (key_matrix.shape[0] // layer_input.shape[1]) * (kv_width // HEAD_SIZE)

    def cut(array):
        return array.reshape(parts, rows_here // parts, array.shape[1])

    query_grad, input_grad, key_weight, value_weight = step(
        seq_count,
        cut(query_rows),
        cut(output_grad),
        cut(key_rows),
        cut(stored_value_rows),
        run_placement,
        cut(layer_input),
        key_matrix,
        value_matrix,
    )
    query_grad, input_grad, key_weight, value_weight = deliver(
        query_grad, input_grad, key_weight, value_weight
    )
    return (query_grad.reshape(query_rows.shape), input_grad, key_weight, value_weight)


def solution(mesh):
    placed = (P("seq", "tp"),) * 5 + (P(None, "tp"), P(None, "tp"), P())
    return jax.shard_map(
        local,
        mesh=mesh,
        in_specs=placed,
        out_specs=(P("seq", "tp"),) * 4,
        check_vma=False,
    )
```

```python
import math

import jax
import jax.numpy as jnp
from jax import lax
from jax.experimental import pallas as pl
from jax.experimental.pallas import tpu as pltpu
from jax.sharding import PartitionSpec as P

HEAD_SIZE = 128
WINDOW_LENGTH = 4096
GROUP = 4
CHUNK = 512
MASKED = -1e30
NT = (((1,), (1,)), ((), ()))
NN = (((1,), (0,)), ((), ()))
TN = (((0,), (0,)), ((), ()))
MESH = pl.DeviceIdType.MESH


def dot(a, b, dims):
    return lax.dot_general(a, b, dims, preferred_element_type=jnp.float32)


def flip(index, bit):
    return index + bit - 2 * bit * ((index // bit) % 2)


def visible(parts, keys):
    return [
        (a, b)
        for a in range(parts)
        for b in range(a + 1)
        if (a - b - 1) * keys + 1 < WINDOW_LENGTH
    ]


def step_kernel(
    q_in, g_in, k_in, v_in, place_in, x_ref, km_ref, vm_ref,
    dq_out, ig_out, kw_out, vw_out,
    kv_ref, qb_ref, gb_ref, kpos_ref, s_ref, dp_ref, p_ref, ds_ref, dqb_ref, dqa_ref,
    sum_ref, give_ref, take_ref, land_ref, wk_ref, xs_ref, acc_ref,
    own_ref, out_ref, got_ref, near_ref, far_ref, dq_ref, ig_ref, kw_ref, vw_ref, q_ref, g_ref, k_ref, v_ref, pos_ref, place_ref,
    plane_send, kv_recv, kvz_send, kvp_send, kvp_recv, qg_send, qg_recv,
    x_sent, x_recv, side_send, side_recv, local_sem,
    give_send, give_recv, z_send, z_recv,
    xp_send, xr_recv, xd_send, xd_recv, wk_send, wk_recv, own_sem, share_sem,
    dq_send, dq_recv,
):
    n = lax.axis_size("seq")
    cores = lax.axis_size("tp")
    me = lax.axis_index("seq")
    tp = lax.axis_index("tp")
    parts, run, _ = q_ref.shape
    kv_local = k_ref.shape[2] // HEAD_SIZE
    plane = cores * kv_local
    pair = GROUP // cores
    depth = n // plane
    z = me // plane
    p = me % plane
    home = p // kv_local
    lane = p % kv_local
    block = plane * run
    keys = n * run
    wide = pair * block
    sub = min(keys, CHUNK)
    roomy = dp_ref.shape[0] > 1
    windowed = parts * keys > WINDOW_LENGTH
    features = x_ref.shape[2]
    x_width = xs_ref.shape[2]
    scale = 1.0 / math.sqrt(HEAD_SIZE)
    power = scale * math.log2(math.e)
    other = {"seq": me, "tp": 1 - tp}

    owner = home == tp
    guest = jnp.logical_not(owner)

    def when(cond, action):
        if cond is None:
            action()
        else:
            pl.when(cond)(action)

    def send(src, dst, send_sem, recv_sem, device, cond=None):
        def copy():
            return pltpu.make_async_remote_copy(
                src_ref=src, dst_ref=dst, send_sem=send_sem, recv_sem=recv_sem,
                device_id=device, device_id_type=MESH,
            )

        when(cond, lambda: copy().start())

    def left(src, send_sem, cond=None):
        def wait():
            pltpu.make_async_remote_copy(
                src_ref=src, dst_ref=src, send_sem=send_sem, recv_sem=send_sem,
                device_id=other, device_id_type=MESH,
            ).wait_send()

        when(cond, wait)

    def arrive(dst, recv_sem, cond=None):
        def wait():
            pltpu.make_async_remote_copy(
                src_ref=dst, dst_ref=dst, send_sem=recv_sem, recv_sem=recv_sem,
                device_id=other, device_id_type=MESH,
            ).wait_recv()

        when(cond, wait)

    def rows_of(index, count):
        return pl.ds(pl.multiple_of(index * count, count), count)

    def lanes_of(index):
        return pl.ds(pl.multiple_of(index * HEAD_SIZE, HEAD_SIZE), HEAD_SIZE)

    bits = [1 << e for e in range(depth.bit_length() - 1)]
    order = sorted(range(depth), key=lambda k: (bin(k).count("1"), -k))

    def layer(k):
        index = z
        for bit in bits:
            if k & bit:
                index = flip(index, bit)
        return index

    def lower(k):
        return [bit for bit in reversed(bits) if k == 0 or bit < (k & -k)]

    layers = depth // cores
    holder = tp == z // layers
    flips = ((1,), (2,), (1, 2))

    def block_of(source):
        return xs_ref.at[:, rows_of(source, run), :]

    def columns_of(target):
        start = (target % layers) * x_width
        return x_ref.at[:, :, pl.ds(pl.multiple_of(start, x_width), x_width)]

    staged = []
    for src, dst in (
        (k_in, k_ref), (v_in, v_ref), (q_in, q_ref), (g_in, g_ref), (place_in, place_ref)
    ):
        staged.append(pltpu.make_async_copy(src, dst, local_sem.at[3 + len(staged)]))
        staged[-1].start()

    own_columns = pltpu.make_async_copy(columns_of(z), block_of(me), local_sem.at[2])
    pl.when(holder)(own_columns.start)

    def x_send(slot, phase):
        target = jnp.where(tp == 0, layers - 1 - slot, tp * layers + slot)
        clear = (target > z) == (z % 2 == 1)
        outer = ((target == 0) | (target == depth - 1)) & (jnp.abs(target - z) > 1)
        now = outer
        if phase < 2:
            now = jnp.logical_not(outer) & (clear if phase == 0 else jnp.logical_not(clear))
        send(
            columns_of(target), block_of(me), x_sent, x_recv.at[z],
            {"seq": target * plane + p, "tp": tp}, (target != z) & now,
        )

    def turned(index, ways):
        for bit in ways:
            index = flip(index, bit)
        return index

    def x_push(k):
        block = block_of(layer(k) * plane + p)
        if k == 0:
            pl.when(holder)(own_columns.wait)
        else:
            arrive(block, x_recv.at[layer(k)], holder)
        for way, ways in enumerate(flips):
            send(block, block, xp_send, xr_recv.at[way, k],
                 {"seq": z * plane + turned(p, ways), "tp": tp}, holder)
        send(block, block, xd_send, xd_recv, other, holder)

    def x_relay(k):
        for way, ways in enumerate(flips):
            block = block_of(layer(k) * plane + turned(p, ways))
            arrive(block, xr_recv.at[way, k], holder)
            send(block, block, xd_send, xd_recv, other, holder)

    barrier = pltpu.get_barrier_semaphore()
    for step in range(n):
        for core in range(cores):
            if step or core:
                pl.semaphore_signal(
                    barrier,
                    inc=1,
                    device_id={"seq": (me + step) % n, "tp": (tp + core) % cores},
                    device_id_type=MESH,
                )
    pl.semaphore_wait(barrier, n * cores - 1)

    for copy in staged:
        copy.wait()

    def piece(role, source):
        return kv_ref.at[role, :, rows_of(source, run), :]

    for i in range(kv_local):
        head = tp * kv_local + i
        target = z * plane + head
        for role, ref in enumerate((k_ref, v_ref)):
            mine = (head == p) & (tp == role)
            cols = slice(i * HEAD_SIZE, (i + 1) * HEAD_SIZE)
            send(
                ref.at[:, :, cols], piece(role, me), plane_send.at[i, role], kv_recv.at[me],
                {"seq": target, "tp": role}, jnp.logical_not(mine),
            )

            @pl.when(mine)
            def _():
                kv_ref[role, :, rows_of(me, run), :] = ref[:, :, cols]

    for i in range(kv_local):
        head = tp * kv_local + i
        target = z * plane + head
        for u in range(cores):
            mine = (head == p) & (tp == u)
            for h in range(pair):
                first = (i * GROUP + u * pair + h) * HEAD_SIZE
                cols = slice(first, first + HEAD_SIZE)
                for w, (ref, buf) in enumerate(((q_ref, qb_ref), (g_ref, gb_ref))):
                    send(
                        ref.at[:, :, cols], buf.at[:, h, rows_of(p, run), :],
                        qg_send.at[w], qg_recv.at[w],
                        {"seq": target, "tp": u}, jnp.logical_not(mine),
                    )

                    @pl.when(mine)
                    def _():
                        buf[:, h, rows_of(p, run), :] = ref[:, :, cols]

    x_push(0)

    short = parts * run // n
    count = run // short
    column = lax.broadcasted_iota(jnp.int32, (n, block), 1)
    row = lax.broadcasted_iota(jnp.int32, (n, block), 0)
    slot = column % run // short
    table = place_ref[...].astype(jnp.bfloat16)
    for s in range(depth):
        picks = (row == s * plane + column // run).astype(jnp.bfloat16)
        slots = dot(table, picks, NN)
        for a in range(parts):
            chosen = jnp.where(row == a * count + slot, slots, 0.0)
            start = (a * count + slot[:1]) * (parts * run) + column[:1] % short
            pos_ref[s * parts + a : s * parts + a + 1, :] = (
                jnp.sum(chosen, axis=0, keepdims=True) * short + start.astype(jnp.float32)
            )
    pos_t = jnp.transpose(pos_ref[...])
    for b in range(parts):
        for s in range(depth):
            column = pos_t[:, s * parts + b : s * parts + b + 1]
            kpos_ref[b, s * block : (s + 1) * block, :] = jnp.broadcast_to(column, (block, block))

    def pass_on(k):
        for j in range(plane):
            source = layer(k) * plane + (p + j) % plane
            place = piece(tp, source)
            arrive(place, kv_recv.at[source], home != tp if k + j == 0 else None)
            for bit in lower(k):
                send(place, place, kvz_send, kv_recv.at[source],
                     {"seq": flip(z, bit) * plane + p, "tp": tp})
            send(place, place, kvp_send, kvp_recv, other)

    relayed = [k for k in order if lower(k)]
    pass_on(0)
    for slot in range(layers):
        x_send(slot, 0)
    for k in relayed[1:]:
        pass_on(k)

    def half_of(src, core):
        return src.at[pl.ds(pl.multiple_of(core * features, features), features), :]

    nearby = []
    for i, src in enumerate((km_ref, vm_ref)):
        send(half_of(src, 1 - tp), far_ref.at[i], side_send.at[i], side_recv.at[i], other)
        nearby.append(pltpu.make_async_copy(half_of(src, tp), near_ref.at[i], local_sem.at[i]))
        nearby[-1].start()

    for slot in range(layers):
        x_send(slot, 1)

    for k in order:
        if k not in relayed:
            pass_on(k)

    fewer = (plane - 1) * run
    for w, buf in enumerate((qb_ref, gb_ref)):
        arrive(buf, qg_recv.at[w], guest)
        arrive(buf.at[:, :, :fewer, :], qg_recv.at[w], owner)
    arrive(kv_ref.at[1 - tp], kvp_recv)

    tiles = visible(parts, keys)

    def lowest(a):
        return min(b for c, b in tiles if c == a)

    where = {tile: t for t, tile in enumerate(tiles)}

    def sweep(body, carry):
        if keys == sub:
            return body(slice(0, keys), carry)
        return lax.fori_loop(0, keys // sub, lambda i, c: body(rows_of(i, sub), c), carry)

    for slot in range(layers):
        x_send(slot, 2)
    x_relay(0)
    inverse, delta = [], []
    for a in range(parts):
        qa = qb_ref[a].reshape(wide, HEAD_SIZE)
        ga = gb_ref[a].reshape(wide, HEAD_SIZE)
        qpos = pos_ref[pl.ds(z * parts + a, 1), :]
        lows = range(lowest(a), a + 1)
        top = jnp.full((1, wide), MASKED, jnp.float32)
        for b in lows:

            def scores(at, top):
                s = dot(kv_ref[0, b, at, :], qa, NT)
                if a == b or windowed:
                    kpos = kpos_ref[b, at, :]
                    seen = kpos <= qpos
                    if windowed:
                        seen = seen & (kpos > qpos - WINDOW_LENGTH)
                    s = jnp.concatenate(
                        [
                            jnp.where(seen, s[:, h * block : (h + 1) * block], MASKED)
                            for h in range(pair)
                        ],
                        axis=1,
                    )
                s_ref[where[a, b], at, :] = s
                return jnp.maximum(top, jnp.max(s, axis=0, keepdims=True))

            top = sweep(scores, top)
        carry = (jnp.zeros((1, wide), jnp.float32), jnp.zeros((1, wide), jnp.float32))
        for b in lows:

            def sums(at, carry):
                total, weighted = carry
                e = jnp.exp2((s_ref[where[a, b], at, :] - top) * power)
                dp = dot(kv_ref[1, b, at, :], ga, NT)
                s_ref[where[a, b], at, :] = e
                if roomy:
                    dp_ref[where[a, b], at, :] = dp
                return (
                    total + jnp.sum(e, axis=0, keepdims=True),
                    weighted + jnp.sum(e * dp, axis=0, keepdims=True),
                )

            carry = sweep(sums, carry)
        total, weighted = carry
        inverse.append(1.0 / total)
        delta.append(weighted / total)

    def backward(b):
        uppers = [a for a in range(parts) if (a, b) in where]
        lo, hi = uppers[0], uppers[-1] + 1
        d = b if roomy else 0
        for a in uppers:
            lanes = slice(a * wide, (a + 1) * wide)

            def grads(at, carry):
                prob = s_ref[where[a, b], at, :] * inverse[a]
                if roomy:
                    dp = dp_ref[where[a, b], at, :]
                else:
                    dp = dot(kv_ref[1, b, at, :], gb_ref[a].reshape(wide, HEAD_SIZE), NT)
                p_ref[at, lanes] = prob.astype(jnp.bfloat16)
                ds_ref[d, at, lanes] = (prob * (dp - delta[a])).astype(jnp.bfloat16)
                return carry

            sweep(grads, 0)
        lanes = slice(lo * wide, hi * wide)
        q_all = qb_ref[lo:hi].reshape((hi - lo) * wide, HEAD_SIZE)
        g_all = gb_ref[lo:hi].reshape((hi - lo) * wide, HEAD_SIZE)

        def products(at, carry):
            dk = dot(ds_ref[d, at, lanes], q_all, NN) * scale
            dv = dot(p_ref[at, lanes], g_all, NN)
            first = tp == 0
            sum_ref[b, at, :] = jnp.where(first, dk, dv)
            give_ref[b, at, :] = jnp.where(first, dv, dk).astype(jnp.bfloat16)
            return carry

        sweep(products, 0)
        send(give_ref.at[b], take_ref.at[b], give_send, give_recv.at[b], other)
        if not roomy:
            for a in uppers:
                query_sum(a, b)

    def query_sum(a, b):
        d = b if roomy else 0
        lanes = slice(a * wide, (a + 1) * wide)

        def add(at, acc):
            return acc + dot(kv_ref[0, b, at, :], ds_ref[d, at, lanes], TN)

        acc = sweep(add, jnp.zeros((HEAD_SIZE, wide), jnp.float32))
        if b == a:
            dqa_ref[a] = acc
        else:
            dqa_ref[a] += acc

    def exchange(b, e):
        bit = bits[e]
        first = depth - depth // bit
        for t in range(depth // (2 * bit)):
            to = flip(z, bit) % (2 * bit) + t * 2 * bit
            rows = rows_of(to, block)
            take_ref[b, rows, :] = sum_ref[b, rows, :].astype(jnp.bfloat16)
            send(
                take_ref.at[b, rows, :], land_ref.at[b, first + t], z_send,
                z_recv.at[b, e], {"seq": flip(z, bit) * plane + p, "tp": tp},
            )

    def cross(b):
        arrive(take_ref.at[b], give_recv.at[b])
        sum_ref[b] += take_ref[b].astype(jnp.float32)
        exchange(b, 0)

    def add_landed(b, e):
        bit = bits[e]
        count = depth // (2 * bit)
        first = depth - depth // bit
        arrive(land_ref.at[b, first : first + count], z_recv.at[b, e])
        for t in range(count):
            rows = rows_of(z % (2 * bit) + t * 2 * bit, block)
            sum_ref[b, rows, :] += land_ref[b, first + t].astype(jnp.float32)

    def fold(e):
        def go(b):
            add_landed(b, e - 1)
            exchange(b, e)

        return go

    def finish(b):
        add_landed(b, len(bits) - 1)
        rows = rows_of(z, block)
        wk_ref[b, rows, :] = sum_ref[b, rows, :].astype(jnp.bfloat16)
        carry(b, 0)

    def carry(b, k):
        place = wk_ref.at[b, rows_of(layer(k), block), :]
        for bit in lower(k):
            send(place, place, wk_send, wk_recv.at[b, layer(k)],
                 {"seq": flip(z, bit) * plane + p, "tp": tp})

    def collect(b, k):
        arrive(wk_ref.at[b, rows_of(layer(k), block), :], wk_recv.at[b, layer(k)])

    def hand(b):
        for k in relayed[1:]:
            collect(b, k)
            carry(b, k)

    def gather(b):
        for k in order:
            if k not in relayed:
                collect(b, k)

    def weigh(b, first):
        part = dot(wk_ref[b], xs_ref[b], TN)
        if first:
            acc_ref[...] = part
        else:
            acc_ref[...] += part

    def own_send():
        for j in range(plane):
            src = wk_ref.at[:, rows_of(z * plane + j, run), :]
            for core in range(cores):
                mine = (p == j) & (tp == core)
                index = tp * plane + p
                send(src, own_ref.at[index], own_sem.at[0], own_sem.at[1],
                     {"seq": z * plane + j, "tp": core}, jnp.logical_not(mine))

                @pl.when(mine)
                def _():
                    own_ref[index] = wk_ref[:, rows_of(z * plane + j, run), :]

    def share():
        grads = jnp.transpose(acc_ref[...]).astype(jnp.bfloat16)
        rows = grads.shape[0] // plane
        for j in range(plane):
            out_ref[j] = grads[j * rows : (j + 1) * rows]
        for ways in ((1, 2), (1,), (2,), ()):
            j = turned(p, ways)
            send(out_ref.at[j], got_ref.at[tp * kv_local + lane], share_sem.at[0], share_sem.at[1],
                 {"seq": z * plane + j, "tp": home}, None if ways else guest)

        @pl.when(owner)
        def _():
            got_ref[tp * kv_local + lane] = out_ref[p]

    def queries():
        for a in range(parts):
            if roomy:
                for b in reversed(range(lowest(a), a + 1)):
                    query_sum(a, b)
            out = (jnp.transpose(dqa_ref[a]) * scale).astype(jnp.bfloat16)
            dqb_ref[a] = out.reshape(pair, block, HEAD_SIZE)
        for j in range(plane):
            for h in range(pair):
                cols = lanes_of(lane * GROUP + tp * pair + h)
                mine = (p == j) & (home == tp)
                src = dqb_ref.at[:, h, j * run : (j + 1) * run, :]
                send(
                    src, dq_ref.at[:, :, cols], dq_send, dq_recv,
                    {"seq": z * plane + j, "tp": home}, jnp.logical_not(mine),
                )

                @pl.when(mine)
                def _():
                    dq_ref[:, :, cols] = dqb_ref[:, h, j * run : (j + 1) * run, :]

    leaving = []

    def put(src, dst):
        leaving.append(pltpu.make_async_copy(src, dst, local_sem.at[8 + len(leaving)]))
        leaving[-1].start()

    def answers():
        arrive(dqb_ref, dq_recv, guest)
        arrive(dqb_ref.at[:, :, :fewer, :], dq_recv, owner)
        put(dq_ref, dq_out)

    def inputs():
        for copy in nearby:
            copy.wait()
        for i in range(2):
            arrive(far_ref.at[i], side_recv.at[i])
        arrive(own_ref.at[: cores * plane - 1], own_sem.at[1])
        rows = parts * run
        grads = [
            own_ref[role * plane + core * kv_local + i].reshape(rows, HEAD_SIZE)
            for core in (tp, 1 - tp)
            for role in range(2)
            for i in range(kv_local)
        ]
        grads = jnp.concatenate(grads, axis=1)
        for f in range(0, features, CHUNK):
            tile = slice(f, min(f + CHUNK, features))
            weights = [ref[i, tile, :] for ref in (near_ref, far_ref) for i in range(2)]
            out = dot(grads, jnp.concatenate(weights, axis=1), NT)
            ig_ref[:, tile] = out.astype(jnp.bfloat16)
        put(ig_ref, ig_out)

    last = parts - 1
    for b in reversed(range(parts)):
        backward(b)
        if b < last:
            cross(b + 1)
        if b == last - 1:
            x_push(1)
        if b == 0:
            for k in range(2, depth):
                x_push(k)
    cross(0)
    stages = [fold(e) for e in range(1, len(bits))] + [finish, hand]
    for tick in range(last + len(stages)):
        for level, stage in enumerate(stages):
            b = last - (tick - level)
            if 0 <= b <= last:
                stage(b)
        if tick == last:
            x_relay(1)
        if tick == last + len(stages) - 2:
            own_send()
            for k in range(2, depth):
                x_relay(k)
            queries()
    arrive(xs_ref, xd_recv, jnp.logical_not(holder))
    for b in reversed(range(parts)):
        gather(b)
        weigh(b, b == last)
    share()
    inputs()
    answers()
    arrive(got_ref, share_sem.at[1], guest)
    arrive(got_ref.at[: cores * kv_local - 1], share_sem.at[1], owner)
    for role, (held, out) in enumerate(((kw_ref, kw_out), (vw_ref, vw_out))):
        for i in range(kv_local):
            cols = slice(i * HEAD_SIZE, (i + 1) * HEAD_SIZE)
            held[:, cols] = got_ref[role * kv_local + i].astype(jnp.float32)
        put(held, out)
    for i in range(kv_local):
        for role in range(cores):
            mine = (tp * kv_local + i == p) & (tp == role)
            left(piece(role, me), plane_send.at[i, role], jnp.logical_not(mine))
    for w, buf in ((0, qb_ref), (1, gb_ref)):
        left(buf, qg_send.at[w], guest)
        left(buf.at[:, :, :fewer, :], qg_send.at[w], owner)
    moves = sum(len(lower(k)) for k in order)
    left(kv_ref.at[0, :, : moves * block, :], kvz_send)
    left(kv_ref.at[0], kvp_send)
    left(xs_ref.at[:, : layers * run, :], x_sent, jnp.logical_not(holder))
    left(xs_ref.at[:, : (layers - 1) * run, :], x_sent, holder)
    left(xs_ref.at[:, : len(flips) * depth * run, :], xp_send, holder)
    left(xs_ref, xd_send, holder)
    for i in range(2):
        left(far_ref.at[i], side_send.at[i])
    left(give_ref, give_send)
    left(take_ref.at[:, : (depth - 1) * block, :], z_send)
    left(dqb_ref, dq_send, guest)
    left(dqb_ref.at[:, :, :fewer, :], dq_send, owner)
    left(wk_ref.at[:, : moves * block, :], wk_send)
    left(own_ref.at[: cores * plane - 1], own_sem.at[0])
    left(out_ref, share_sem.at[0], guest)
    left(out_ref.at[: plane - 1], share_sem.at[0], owner)
    for copy in leaving:
        copy.wait()


def deliver_kernel(*refs):
    count = (len(refs) - 1) // 3
    ins, outs, held = refs[:count], refs[count : 2 * count], refs[2 * count : 3 * count]
    moves = []
    for i in range(count):
        moves.append(pltpu.make_async_copy(ins[i], held[i], refs[-1].at[0, i]))
        moves[-1].start()
    for i in range(count):
        moves[i].wait()
        moves.append(pltpu.make_async_copy(held[i], outs[i], refs[-1].at[1, i]))
        moves[-1].start()
    for move in moves[count:]:
        move.wait()


def deliver(*arrays):
    hbm = pl.BlockSpec(memory_space=pl.ANY)
    count = len(arrays)
    return pl.pallas_call(
        deliver_kernel,
        out_shape=tuple(jax.ShapeDtypeStruct(a.shape, a.dtype) for a in arrays),
        in_specs=[hbm] * count,
        out_specs=(hbm,) * count,
        scratch_shapes=[pltpu.VMEM(a.shape, a.dtype) for a in arrays]
        + [pltpu.SemaphoreType.DMA((2, count))],
    )(*arrays)


def step(n, q, g, k, v, place, x, km, vm):
    parts, run, width = q.shape
    kv_width = k.shape[2]
    kv_local = kv_width // HEAD_SIZE
    features = x.shape[2]
    heads = width // HEAD_SIZE
    cores = km.shape[0] // features
    plane = cores * kv_local
    pair = GROUP // cores
    depth = n // plane
    levels = depth.bit_length() - 1
    block = plane * run
    keys = n * run
    wide = pair * block
    block_width = cores * features // n
    x_width = plane * block_width
    roomy = parts * keys <= 4096
    tiles = len(visible(parts, keys))
    hbm = pl.BlockSpec(memory_space=pl.ANY)
    kind = jnp.bfloat16
    real = jnp.float32
    dma = pltpu.SemaphoreType.DMA
    return pl.pallas_call(
        step_kernel,
        out_shape=(
            jax.ShapeDtypeStruct((parts, run, width), kind),
            jax.ShapeDtypeStruct((parts * run, features), kind),
            jax.ShapeDtypeStruct((block_width, kv_width), real),
            jax.ShapeDtypeStruct((block_width, kv_width), real),
        ),
        in_specs=[hbm] * 8,
        out_specs=(hbm,) * 4,
        scratch_shapes=[
            pltpu.VMEM((2, parts, keys, HEAD_SIZE), kind),
            pltpu.VMEM((parts, pair, block, HEAD_SIZE), kind),
            pltpu.VMEM((parts, pair, block, HEAD_SIZE), kind),
            pltpu.VMEM((parts, keys, block), real),
            pltpu.VMEM((tiles, keys, wide), real),
            pltpu.VMEM((tiles, keys, wide) if roomy else (1, 8, 128), real),
            pltpu.VMEM((keys, parts * wide), kind),
            pltpu.VMEM((parts if roomy else 1, keys, parts * wide), kind),
            pltpu.VMEM((parts, pair, block, HEAD_SIZE), kind),
            pltpu.VMEM((parts, HEAD_SIZE, wide), real),
            pltpu.VMEM((parts, keys, HEAD_SIZE), real),
            pltpu.VMEM((parts, keys, HEAD_SIZE), kind),
            pltpu.VMEM((parts, keys, HEAD_SIZE), kind),
            pltpu.VMEM((parts, depth - 1, block, HEAD_SIZE), kind),
            pltpu.VMEM((parts, keys, HEAD_SIZE), kind),
            pltpu.VMEM((parts, keys, x_width), kind),
            pltpu.VMEM((HEAD_SIZE, x_width), real),
            pltpu.VMEM((cores * plane, parts, run, HEAD_SIZE), kind),
            pltpu.VMEM((plane, block_width, HEAD_SIZE), kind),
            pltpu.VMEM((cores * kv_local, block_width, HEAD_SIZE), kind),
            pltpu.VMEM((2, features, kv_width), kind),
            pltpu.VMEM((2, features, kv_width), kind),
            pltpu.VMEM((parts, run, width), kind),
            pltpu.VMEM((parts * run, features), kind),
            pltpu.VMEM((block_width, kv_width), real),
            pltpu.VMEM((block_width, kv_width), real),
            pltpu.VMEM((parts, run, width), kind),
            pltpu.VMEM((parts, run, width), kind),
            pltpu.VMEM((parts, run, kv_width), kind),
            pltpu.VMEM((parts, run, kv_width), kind),
            pltpu.VMEM((depth * parts, block), real),
            pltpu.VMEM((n, n), jnp.int32),
            dma((kv_local, cores)),
            dma((n,)),
            dma,
            dma,
            dma,
            dma((2,)),
            dma((2,)),
            dma,
            dma((depth,)),
            dma((2,)),
            dma((2,)),
            dma((12,)),
            dma,
            dma((parts,)),
            dma,
            dma((parts, levels)),
            dma,
            dma((3, depth)),
            dma,
            dma,
            dma,
            dma((parts, depth)),
            dma((2,)),
            dma((2,)),
            dma,
            dma,
        ],
        compiler_params=pltpu.CompilerParams(
            vmem_limit_bytes=63 * 2**20, collective_id=0, has_side_effects=True
        ),
    )(q, g, k, v, place, x, km, vm)


def local(
    query_rows,
    key_rows,
    stored_value_rows,
    output_grad,
    layer_input,
    key_matrix,
    value_matrix,
    run_placement,
):
    seq_index = lax.axis_index("seq")
    seq_count = run_placement.shape[0]
    rows_here = query_rows.shape[0]
    kv_width = key_rows.shape[1]
    parts = (key_matrix.shape[0] // layer_input.shape[1]) * (kv_width // HEAD_SIZE)

    def cut(array):
        return array.reshape(parts, rows_here // parts, array.shape[1])

    query_grad, input_grad, key_weight, value_weight = step(
        seq_count,
        cut(query_rows),
        cut(output_grad),
        cut(key_rows),
        cut(stored_value_rows),
        run_placement,
        cut(layer_input),
        key_matrix,
        value_matrix,
    )
    query_grad, input_grad, key_weight, value_weight = deliver(
        query_grad, input_grad, key_weight, value_weight
    )
    return (query_grad.reshape(query_rows.shape), input_grad, key_weight, value_weight)


def solution(mesh):
    placed = (P("seq", "tp"),) * 5 + (P(None, "tp"), P(None, "tp"), P())
    return jax.shard_map(
        local,
        mesh=mesh,
        in_specs=placed,
        out_specs=(P("seq", "tp"),) * 4,
        check_vma=False,
    )
```
